128 devices in a mesh: edp: 2 (over z_lo), ep: 64 (over z_hi, x, y, core).
Axes of the slice: x: 4, y: 4, z: 4 (z_hi: 2, z_lo: 2; z = z_hi * 2 + z_lo), core: 2. Of those that a mesh axis runs over, the one named last changes fastest.
Arguments:
- tokens: bfloat16 [16384, 3584], P(('edp', 'ep')), may hold values from -6 to 6
- node_ids: int32 [16384, 4], P(('edp', 'ep')), may hold values from 0 to 7, as said below
- local_ids: int32 [16384, 8], P(('edp', 'ep')), may hold values from 0 to 15, as said below
- affinity: float32 [16384, 8], P(('edp', 'ep')), may hold values from 0.2 to 1
- w_gate: bfloat16 [128, 3584, 1024], P(('edp', 'ep')), may hold values from -0.09375 to 0.09375
- w_up: bfloat16 [128, 3584, 1024], P(('edp', 'ep')), may hold values from -0.09375 to 0.09375
- w_down: bfloat16 [128, 1024, 3584], P(('edp', 'ep')), may hold values from -0.1875 to 0.1875
- grad_parts: float32 [128, 3584, 128], P(('edp', 'ep')), may hold values from -2.5 to 2.5
Outputs:
- mixed: bfloat16 [16384, 3584], P(('edp', 'ep'))
- router_grad: float32 [3584, 128], P(('edp', 'ep'))
The draws below stay inside these ranges and needn't reach their ends.
Inputs may be any that keep to these rules, and one draw needn't show every extreme that they name: `node_ids`: A token's 4 nodes are distinct and increasing. `local_ids`: columns 2 j and 2 j + 1 name the two experts 2 m and 2 m + 1 of one pair m of node node_ids[t, j], in either order. From the 128 tokens of one device each expert receives at most 10 routes; inside a node the loads from one device differ by at most one.
All inputs are finite; a program needn't handle non-finite values.
Results may differ from the reference program's by a relative error of at most 0.0057.
Values may be sent and summed in bfloat16 or wider, within the bound.
No kernel may reach another device: no remote copies, remote signals or barrier semaphores. Data moves between devices by JAX's collectives and lax.ppermute only.
A program may use at most 192 MiB of HBM per device.

```python
import math
import jax
import jax.numpy as jnp
from jax import lax

D = 3584
H = 1024
TOK_DEV = 128
TOP = 8
NODE_PICK = 4
GROUPS = 8
EXPERTS = 128
CAP = 10
TOKENS = 16384
N_EDP = 2
N_EP = 64


def routing_plan(key):
    base_key = jax.random.fold_in(key, 7)
    per_node = EXPERTS // GROUPS
    pair_count = per_node // 2
    pairing = jax.random.permutation(jax.random.fold_in(base_key, 1), GROUPS).astype(jnp.int32)

    def block_plan(block):
        block_key = jax.random.fold_in(base_key, block + 100)
        shifts = jax.random.randint(jax.random.fold_in(block_key, 1), (GROUPS // 2,), 0, TOK_DEV // 8 + 1).astype(jnp.int32)
        shifts = shifts.at[0].set(TOK_DEV // 8)
        counts = jnp.zeros((GROUPS,), jnp.int32)
        counts = counts.at[pairing[0::2]].set(TOK_DEV // 2 + shifts)
        counts = counts.at[pairing[1::2]].set(TOK_DEV // 2 - shifts)
        node_major = jnp.repeat(jnp.arange(GROUPS, dtype=jnp.int32), counts, total_repeat_length=NODE_PICK * TOK_DEV)
        chosen = node_major.reshape(NODE_PICK, TOK_DEV).T
        shuffle = jax.random.permutation(jax.random.fold_in(block_key, 2), TOK_DEV)
        chosen = chosen[shuffle]
        onehot = jnp.sum((chosen[:, :, None] == jnp.arange(GROUPS, dtype=jnp.int32)[None, None, :]).astype(jnp.int32), axis=1)
        earlier = jnp.cumsum(onehot, axis=0) - onehot
        ranks = jnp.take_along_axis(earlier, chosen, axis=1)
        offsets = jax.random.randint(jax.random.fold_in(block_key, 3), (GROUPS,), 0, pair_count).astype(jnp.int32)
        pair_index = (ranks + offsets[chosen]) % pair_count
        flips = jax.random.randint(jax.random.fold_in(block_key, 4), (TOK_DEV, NODE_PICK), 0, 2).astype(jnp.int32)
        first = 2 * pair_index + flips
        second = 2 * pair_index + 1 - flips
        local = jnp.stack([first, second], axis=2).reshape(TOK_DEV, TOP)
        return (chosen, local)
    nodes, locals_all = jax.vmap(block_plan)(jnp.arange(EXPERTS, dtype=jnp.int32))
    return (nodes.reshape(-1, NODE_PICK).astype(jnp.int32), locals_all.reshape(-1, TOP).astype(jnp.int32))


def draw_node_ids(key, part):
    return routing_plan(key)[0]


def draw_local_ids(key, part):
    return routing_plan(key)[1]


def with_spikes(entries, rng, source, target, blocks, factor):
    def block_of(position):
        return (jnp.arange(entries.shape[position]) // (entries.shape[position] // blocks)).reshape((-1,) + (1,) * (entries.ndim - 1 - position))

    near = jax.random.permutation(rng, blocks)[block_of(target)]
    far = (block_of(target) + blocks // 2) % blocks
    return jnp.where((block_of(source) == near) | (block_of(source) == far), factor * entries, entries)


def level_of(stream_key, dims, split, least, high):
    factor_of, own = 1.0, jax.random.fold_in(stream_key, 6)
    for axis_at, shards_of in split:
        steps = jnp.exp(jax.random.uniform(jax.random.fold_in(own, axis_at), (shards_of,), jnp.float32, least / len(split), high / len(split)))
        factor_of = factor_of * jnp.repeat(steps, dims[axis_at] // shards_of).reshape([-1 if axis == axis_at else 1 for axis in range(len(dims))])
    return factor_of


def bell_draw(stream_key, shape, spread, most, split=(), held_as=jnp.bfloat16):
    level = level_of(stream_key, shape, split, -0.22, 0.18) if split else 1.0
    values = jax.random.normal(stream_key, shape, jnp.float32) * spread * level
    return jnp.minimum(jnp.maximum(values, -most), most).astype(held_as)


def bell_draw_with(stream_key, dims, scale, limit, shards, heavy, kind=jnp.bfloat16):
    entries = scale * jax.random.normal(stream_key, dims, jnp.float32)
    if shards:
        entries = entries * level_of(stream_key, dims, shards, -0.22, 0.18)
    return jnp.clip(with_spikes(entries, jax.random.fold_in(stream_key, 3), *heavy), -limit, limit).astype(kind)


def setup_inputs(seed: int = 0) -> dict:
    keys = jax.random.split(jax.random.key(seed), 9)
    tokens = bell_draw(keys[0], (TOKENS, D), 1.0, 6.0, ((0, 128),))
    node_ids = draw_node_ids(jax.random.fold_in(keys[8], 71), 0)
    local_ids = draw_local_ids(jax.random.fold_in(keys[8], 71), 0)
    affinity = jnp.clip(jnp.exp(math.log(1.0) - 1.609438 * jax.random.uniform(keys[3], (TOKENS, TOP), jnp.float32) ** level_of(keys[3], (TOKENS, TOP), ((0, 128),), -0.2, 0.2)), 0.2, 1.0)
    w_gate = bell_draw(keys[4], (EXPERTS, D, H), D ** -0.5, 0.09375, ((0, 128),))
    w_up = bell_draw(keys[5], (EXPERTS, D, H), D ** -0.5, 0.09375, ((0, 128),))
    w_down = bell_draw(keys[6], (EXPERTS, H, D), H ** -0.5, 0.1875, ((0, 128),))
    grad_parts = bell_draw_with(keys[7], (N_EDP * N_EP, D, EXPERTS), 0.1, 2.5, ((0, 128),), (0, 1, 128, 5.5), jnp.float32)
    return {"tokens": tokens, "node_ids": node_ids, "local_ids": local_ids, "affinity": affinity, "w_gate": w_gate, "w_up": w_up, "w_down": w_down, "grad_parts": grad_parts}


def reference(tokens, node_ids, local_ids, affinity, w_gate, w_up, w_down, grad_parts):
    per_node = EXPERTS // GROUPS
    expert = (jnp.repeat(node_ids, 2, axis=1) * per_node + local_ids).astype(jnp.int32)
    weight = 2.5 * affinity / jnp.sum(affinity, axis=1, keepdims=True)
    flat_expert = expert.reshape(-1)
    route_order = jnp.argsort(flat_expert, stable=True).astype(jnp.int32)
    counts = jnp.bincount(flat_expert, length=EXPERTS).astype(jnp.int32)
    starts = (jnp.cumsum(counts) - counts).astype(jnp.int32)
    rows_most = CAP * N_EDP * N_EP
    padded_order = jnp.concatenate([route_order, jnp.zeros((rows_most,), jnp.int32)])
    flat_weight = weight.reshape(-1)

    def per_expert(accum, inputs):
        gate_w, up_w, down_w, start, count = inputs
        row_index = lax.dynamic_slice(padded_order, (start.astype(jnp.int32),), (rows_most,))
        is_valid = jnp.arange(rows_most, dtype=jnp.int32) < count
        token_index = row_index // TOP
        row_block = tokens[token_index]
        gate_act = jnp.dot(row_block, gate_w, preferred_element_type=jnp.float32)
        up_act = jnp.dot(row_block, up_w, preferred_element_type=jnp.float32)
        hidden = (jax.nn.silu(gate_act) * up_act).astype(jnp.bfloat16)
        result = jnp.dot(hidden, down_w, preferred_element_type=jnp.float32).astype(jnp.bfloat16)
        scaled = jnp.where(is_valid, flat_weight[row_index], jnp.zeros((), jnp.float32))
        accum = accum.at[token_index].add(scaled[:, None] * result.astype(jnp.float32))
        return accum, None

    start_sum = jnp.zeros(tokens.shape, jnp.float32)
    mixed_sum, _ = lax.scan(per_expert, start_sum, (w_gate, w_up, w_down, starts, counts))
    router_grad = jnp.sum(grad_parts, axis=0)
    return mixed_sum.astype(jnp.bfloat16), router_grad
```

```python
import jax
import jax.numpy as jnp
from jax import lax
from jax.experimental import pallas as pl
from jax.experimental.pallas import tpu as pltpu
from jax.sharding import Mesh, PartitionSpec as P

PAIRS, HEAD, TAIL, WIDE = 64, 8, 2, 28
SLOTS = HEAD + TAIL
TAIL_AT, COEF_AT = HEAD * WIDE, SLOTS * WIDE
IN_ROWS = COEF_AT + 8
F32, BF16, I32 = jnp.float32, jnp.bfloat16, jnp.int32


def iota(shape, dim):
    return lax.broadcasted_iota(I32, shape, dim)


def pair_of(node_ref, local_ref, column):
    return node_ref[column : column + 1, :] * 8 + local_ref[2 * column : 2 * column + 1, :] // 2


def hits(node_ref, local_ref, pair):
    found = jnp.zeros(pair.shape, jnp.bool_)
    for column in range(4):
        found = found | (pair == pair_of(node_ref, local_ref, column))
    return found


def picks(node_ref, local_ref):
    tok = node_ref.shape[1]
    earlier = (iota((tok, tok), 0) < iota((tok, tok), 1)).astype(BF16)
    row = iota((PAIRS * HEAD, tok), 0)
    head_hit = hits(node_ref, local_ref, row // HEAD)
    head_rank = jnp.dot(head_hit.astype(F32).astype(BF16), earlier, preferred_element_type=F32)
    head = jnp.where(head_hit & (head_rank == (row % HEAD).astype(F32)), 1.0, 0.0)
    hit = hits(node_ref, local_ref, iota((PAIRS, tok), 0))
    rank = jnp.dot(hit.astype(F32).astype(BF16), earlier, preferred_element_type=F32)
    each = [jnp.where(hit & (rank == float(slot)), 1.0, 0.0) for slot in range(SLOTS)]
    return head, each


def send_kernel(node_ref, local_ref, aff_ref, tok_ref, out_ref, tail_ref):
    head, each = picks(node_ref, local_ref)
    head = head.astype(BF16)
    tail = jnp.concatenate(each[HEAD:], axis=0).astype(BF16)
    for k in range(7):
        rows = jnp.dot(head, tok_ref[:, 512 * k : 512 * (k + 1)], preferred_element_type=F32)
        for m in range(4):
            j = 4 * k + m
            tile = rows[:, 128 * m : 128 * (m + 1)].reshape(PAIRS, HEAD, 128)
            out_ref[:, 8 * j : 8 * j + 8, :] = tile.astype(BF16)
        rows = jnp.dot(tail, tok_ref[:, 512 * k : 512 * (k + 1)], preferred_element_type=F32)
        for m in range(4):
            for s in range(TAIL):
                tail_ref[pl.ds(s * WIDE + 4 * k + m, PAIRS, stride=TAIL * WIDE), :] = rows[
                    PAIRS * s : PAIRS * (s + 1), 128 * m : 128 * (m + 1)
                ]
    out_ref[:, TAIL_AT:COEF_AT, :] = tail_ref[...].reshape(PAIRS, TAIL * WIDE, 128).astype(BF16)
    aff = aff_ref[...]
    weight = 2.5 * aff / jnp.sum(aff, axis=0, keepdims=True)
    tok = node_ref.shape[1]
    pair = iota((PAIRS, tok), 0)
    even = jnp.zeros((PAIRS, tok), F32)
    odd = jnp.zeros((PAIRS, tok), F32)
    for column in range(4):
        first, second = weight[2 * column : 2 * column + 1, :], weight[2 * column + 1 : 2 * column + 2, :]
        flip = local_ref[2 * column : 2 * column + 1, :] % 2 == 1
        here = pair == pair_of(node_ref, local_ref, column)
        even = jnp.where(here, jnp.where(flip, second, first), even)
        odd = jnp.where(here, jnp.where(flip, first, second), odd)
    lane = iota((PAIRS, 128), 1)
    coef = jnp.zeros((PAIRS, 128), F32)
    for slot in range(SLOTS):
        even_w = jnp.sum(each[slot] * even, axis=1, keepdims=True)
        odd_w = jnp.sum(each[slot] * odd, axis=1, keepdims=True)
        coef = jnp.where(lane // 2 == 2 * slot, even_w, coef)
        coef = jnp.where(lane // 2 == 2 * slot + 1, odd_w, coef)
    high = coef.astype(BF16).astype(F32)
    coef = jnp.where(lane % 2 == 0, high, coef - high)
    out_ref[:, COEF_AT:IN_ROWS, :] = jnp.broadcast_to(coef[:, None, :], (PAIRS, 8, 128)).astype(BF16)


def unpack(in_ref, rows_ref, tail_ref):
    for j in range(WIDE):
        tile = in_ref[:, 8 * j : 8 * j + 8, :].astype(F32).reshape(PAIRS * HEAD, 128)
        rows_ref[: PAIRS * HEAD, 128 * j : 128 * (j + 1)] = tile.astype(BF16)
    tail_ref[...] = in_ref[:, TAIL_AT:COEF_AT, :].astype(F32).reshape(PAIRS * TAIL * WIDE, 128)
    for s in range(TAIL):
        at = PAIRS * (HEAD + s)
        for j in range(WIDE):
            tile = tail_ref[pl.ds(s * WIDE + j, PAIRS, stride=TAIL * WIDE), :]
            rows_ref[at : at + PAIRS, 128 * j : 128 * (j + 1)] = tile.astype(BF16)


def expert_kernel(core_ref, in_ref, gate_ref, up_ref, down_ref, out_ref, rows_ref, hid_ref, w_ref, tail_ref):
    step = pl.program_id(0)

    @pl.when(step == 0)
    def _():
        unpack(in_ref, rows_ref, tail_ref)
        core = core_ref[0]
        coef = in_ref[:, COEF_AT:IN_ROWS, :].astype(F32).reshape(PAIRS * 8, 128)
        tail_ref[: PAIRS * 8, :] = coef
        row, lane = iota((PAIRS * 8, 128), 0), iota((PAIRS * 8, 128), 1)
        mine = jnp.where(lane // 2 == 2 * (row % 8) + core, coef, 0.0)
        w_ref[: PAIRS * HEAD, :] = jnp.broadcast_to(jnp.sum(mine, axis=1, keepdims=True), (PAIRS * 8, 128))
        coef = tail_ref[pl.ds(0, PAIRS, stride=8), :]
        lane = iota((PAIRS, 128), 1)
        for s in range(TAIL):
            mine = jnp.where(lane // 2 == 2 * (HEAD + s) + core, coef, 0.0)
            at = PAIRS * (HEAD + s)
            w_ref[at : at + PAIRS, :] = jnp.broadcast_to(jnp.sum(mine, axis=1, keepdims=True), (PAIRS, 128))

    @pl.when(step < 4)
    def _():
        rows = rows_ref[...]
        gate = jnp.dot(rows, gate_ref[0], preferred_element_type=F32)
        up = jnp.dot(rows, up_ref[0], preferred_element_type=F32)
        hidden = gate / (1.0 + jnp.exp(-gate)) * up
        hid_ref[:, pl.ds(pl.multiple_of(step * 256, 256), 256)] = hidden.astype(BF16)

    @pl.when(step >= 4)
    def _():
        block = step - 4
        value = jnp.dot(hid_ref[...], down_ref[0], preferred_element_type=F32)
        w = w_ref[...]
        for m in range(4):
            part = value[:, 128 * m : 128 * (m + 1)] * w
            tile = part[: PAIRS * HEAD].reshape(PAIRS, HEAD, 128).astype(BF16)
            out_ref[:, pl.ds(pl.multiple_of(32 * block + 8 * m, 8), 8), :] = tile
            for s in range(TAIL):
                at = PAIRS * (HEAD + s)
                tail_ref[pl.ds(s * WIDE + 4 * block + m, PAIRS, stride=TAIL * WIDE), :] = part[at : at + PAIRS]

    @pl.when(step == 10)
    def _():
        out_ref[:, TAIL_AT:COEF_AT, :] = tail_ref[...].reshape(PAIRS, TAIL * WIDE, 128).astype(BF16)


def mix_kernel(node_ref, local_ref, in_ref, out_ref, rows_ref, tail_ref):
    head, each = picks(node_ref, local_ref)
    pick = jnp.concatenate([head] + each[HEAD:], axis=0).astype(BF16)
    unpack(in_ref, rows_ref, tail_ref)
    for k in range(7):
        at = slice(512 * k, 512 * (k + 1))
        value = lax.dot_general(pick, rows_ref[:, at], (((0,), (0,)), ((), ())), preferred_element_type=F32)
        out_ref[:, at] = value.astype(BF16)


def vmem(mib):
    return pltpu.CompilerParams(vmem_limit_bytes=mib << 20)


def body(tokens, node_ids, local_ids, affinity, w_gate, w_up, w_down, grad_parts):
    tok, width = tokens.shape
    nodes, locals_ = node_ids.T, local_ids.T
    tail = pltpu.VMEM((PAIRS * TAIL * WIDE, 128), F32)
    rows = pltpu.VMEM((PAIRS * SLOTS, width), BF16)
    chips = ("edp", "chip")
    message = pl.pallas_call(
        send_kernel,
        out_shape=jax.ShapeDtypeStruct((PAIRS, IN_ROWS, 128), BF16),
        scratch_shapes=[tail],
        compiler_params=vmem(32),
        name="send",
    )(nodes, locals_, affinity.T, tokens)
    own = lax.all_to_all(message, chips, split_axis=0, concat_axis=0, tiled=True)
    swap = [(0, 1), (1, 0)]
    other = lax.ppermute(own, "core", swap)
    core = lax.axis_index("core").astype(I32).reshape(1)
    experts = pl.pallas_call(
        expert_kernel,
        grid=(11,),
        in_specs=[
            pl.BlockSpec(memory_space=pltpu.SMEM),
            pl.BlockSpec((PAIRS, IN_ROWS, 128), lambda i: (0, 0, 0)),
            pl.BlockSpec((1, width, 256), lambda i: (0, 0, jnp.minimum(i, 3))),
            pl.BlockSpec((1, width, 256), lambda i: (0, 0, jnp.minimum(i, 3))),
            pl.BlockSpec((1, 1024, 512), lambda i: (0, 0, jnp.maximum(i - 4, 0))),
        ],
        out_specs=pl.BlockSpec((PAIRS, COEF_AT, 128), lambda i: (0, 0, 0)),
        out_shape=jax.ShapeDtypeStruct((PAIRS, COEF_AT, 128), BF16),
        scratch_shapes=[
            rows,
            pltpu.VMEM((PAIRS * SLOTS, 1024), BF16),
            pltpu.VMEM((PAIRS * SLOTS, 128), F32),
            tail,
        ],
        compiler_params=vmem(56),
        name="experts",
    )
    for_other = experts(core, other, w_gate, w_up, w_down)
    back = lax.ppermute(for_other, "core", swap)
    mine = experts(core, own, w_gate, w_up, w_down)
    both = (mine.astype(F32) + back.astype(F32)).astype(BF16)
    returned = lax.all_to_all(both, chips, split_axis=0, concat_axis=0, tiled=True)
    mixed = pl.pallas_call(
        mix_kernel,
        out_shape=jax.ShapeDtypeStruct((tok, width), BF16),
        scratch_shapes=[rows, tail],
        compiler_params=vmem(32),
        name="mix",
    )(nodes, locals_, returned)
    halves = grad_parts[0].reshape(PAIRS, 2, WIDE, 128)
    first, second = halves[:, 0], halves[:, 1]
    keep = jnp.where(core[0] == 0, first, second)
    give = jnp.where(core[0] == 0, second, first).astype(BF16)
    got = lax.ppermute(give, "core", swap)
    pair_sum = (keep + got.astype(F32)).astype(BF16)
    parts = lax.all_to_all(pair_sum, chips, split_axis=0, concat_axis=0, tiled=True)
    router_grad = parts.astype(F32).sum(axis=0)
    return mixed, router_grad


def solution(mesh):
    split = Mesh(mesh.devices.reshape(2, 32, 2), ("edp", "chip", "core"))
    every = ("edp", "chip", "core")
    flat, deep = P(every, None), P(every, None, None)
    return jax.shard_map(
        body,
        mesh=split,
        in_specs=(flat, flat, flat, flat, deep, deep, deep, deep),
        out_specs=(flat, flat),
        check_vma=False,
    )
```

```python
import functools

import jax
import jax.numpy as jnp
from jax import lax
from jax.experimental import pallas as pl
from jax.experimental.pallas import tpu as pltpu
from jax.sharding import Mesh, PartitionSpec as P

PAIRS, SLOTS, WIDE = 64, 5, 28
COEF_AT = SLOTS * WIDE
MSG = COEF_AT + 4
GRAD = 32
PITCH = MSG + 8
ROWS = PAIRS * SLOTS
F32, BF16, I32 = jnp.float32, jnp.bfloat16, jnp.int32


def iota(shape, dim):
    return lax.broadcasted_iota(I32, shape, dim)


def pair_of(node_ref, local_ref, column):
    return node_ref[column : column + 1, :] * 8 + local_ref[2 * column : 2 * column + 1, :] // 2


def picks(node_ref, local_ref, start):
    tok = node_ref.shape[1]
    pair = iota((PAIRS, tok), 0)
    hit = jnp.zeros((PAIRS, tok), jnp.bool_)
    for column in range(4):
        hit = hit | (pair == pair_of(node_ref, local_ref, column))
    earlier = (iota((tok, tok), 0) < iota((tok, tok), 1)).astype(BF16)
    rank = jnp.dot(hit.astype(F32).astype(BF16), earlier, preferred_element_type=F32)
    return [jnp.where(hit & (rank == float(start + slot)), 1.0, 0.0) for slot in range(SLOTS)]


def lane_tile(j):
    return slice(128 * j, 128 * (j + 1))


def send_kernel(start, node_ref, local_ref, aff_ref, tok_ref, *refs):
    grad_refs, (out_ref, flat_ref) = refs[:-2], refs[-2:]
    each = picks(node_ref, local_ref, start)
    pick = jnp.concatenate(each, axis=0).astype(BF16)
    for k in range(7):
        rows = jnp.dot(pick, tok_ref[:, 512 * k : 512 * (k + 1)], preferred_element_type=F32)
        for m in range(4):
            for s in range(SLOTS):
                at = pl.ds(s * WIDE + 4 * k + m, PAIRS, stride=PITCH)
                flat_ref[at, :] = rows[PAIRS * s : PAIRS * (s + 1), lane_tile(m)]
    aff = aff_ref[...]
    weight = 2.5 * aff / jnp.sum(aff, axis=0, keepdims=True)
    tok = node_ref.shape[1]
    pair = iota((PAIRS, tok), 0)
    even = jnp.zeros((PAIRS, tok), F32)
    odd = jnp.zeros((PAIRS, tok), F32)
    for column in range(4):
        first, second = weight[2 * column : 2 * column + 1, :], weight[2 * column + 1 : 2 * column + 2, :]
        flip = local_ref[2 * column : 2 * column + 1, :] % 2 == 1
        here = pair == pair_of(node_ref, local_ref, column)
        even = jnp.where(here, jnp.where(flip, second, first), even)
        odd = jnp.where(here, jnp.where(flip, first, second), odd)
    lane = iota((PAIRS, 128), 1)
    coef = jnp.zeros((PAIRS, 128), F32)
    for slot in range(SLOTS):
        even_w = jnp.sum(each[slot] * even, axis=1, keepdims=True)
        odd_w = jnp.sum(each[slot] * odd, axis=1, keepdims=True)
        coef = jnp.where(lane // 2 == 2 * slot, even_w, coef)
        coef = jnp.where(lane // 2 == 2 * slot + 1, odd_w, coef)
    high = coef.astype(BF16).astype(F32)
    coef = jnp.where(lane % 2 == 0, high, coef - high)
    for row in range(COEF_AT, MSG):
        flat_ref[pl.ds(row, PAIRS, stride=PITCH), :] = coef
    out_ref[:, :MSG, :] = flat_ref.reshape(PAIRS, PITCH, 128)[:, :MSG, :].astype(BF16)
    if grad_refs:
        keep_ref, got_ref = grad_refs
        out_ref[:, MSG:, :] = (keep_ref[...] + got_ref[...].astype(F32)).astype(BF16)


def halves_kernel(core_ref, in_ref, keep_ref, give_ref):
    blocks = in_ref.reshape(PAIRS, 2 * WIDE, 128)
    first = core_ref[0] == 0
    low, high = blocks[:, :24, :], blocks[:, 32:, :]
    shared = blocks[:, 24:32, :]
    keep_ref[:, :24, :] = jnp.where(first, low, high)
    keep_ref[:, 24:, :] = shared
    give_ref[:, :24, :] = jnp.where(first, high, low).astype(BF16)
    give_ref[:, 24:, :] = shared.astype(BF16)


def spread(src_ref, flat_ref):
    flat_ref.reshape(PAIRS, PITCH, 128)[:, :MSG, :] = src_ref[...].astype(F32)


def lay_out(flat_ref, rows_ref, first, last):
    for s in range(SLOTS):
        for j in range(first, last):
            tile = flat_ref[pl.ds(s * WIDE + j, PAIRS, stride=PITCH), :]
            rows_ref[PAIRS * s : PAIRS * (s + 1), lane_tile(j)] = tile.astype(BF16)


PIECES = ((0, 4), (4, 10), (10, 18), (18, 28))


def expert_kernel(
    core_ref, in_ref, gate_ref, up_ref, down_ref, out_ref,
    msg, flat, rows, gate, up, down, acc, hid, w_ref, sem_in, sem_g, sem_u, sem_d, sem_out,
):
    half = down.shape[1] // 2
    started = {}

    def launch(k):
        if k < len(PIECES):
            at = slice(128 * PIECES[k][0], 128 * PIECES[k][1])
            copies = [
                pltpu.make_async_copy(gate_ref.at[0, at, :], gate.at[at, :], sem_g.at[k]),
                pltpu.make_async_copy(up_ref.at[0, at, :], up.at[at, :], sem_u.at[k]),
            ]
        else:
            n = k - len(PIECES)
            at = slice(half * n, half * (n + 1))
            copies = [pltpu.make_async_copy(down_ref.at[0, :, at], down.at[:, at], sem_d.at[n])]
        for copy in copies:
            copy.start()
        started[k] = copies

    def arrive(k):
        for copy in started[k]:
            copy.wait()

    load = pltpu.make_async_copy(in_ref.at[:, :MSG, :], msg, sem_in.at[0])
    load.start()
    launch(0)
    launch(1)
    load.wait()
    spread(msg, flat)
    lay_out(flat, rows, *PIECES[0])
    core = core_ref[0]
    coef = flat[pl.ds(COEF_AT, PAIRS, stride=PITCH), :]
    lane = iota((PAIRS, 128), 1)
    for s in range(SLOTS):
        mine = jnp.where(lane // 2 == 2 * s + core, coef, 0.0)
        w_ref[PAIRS * s : PAIRS * (s + 1), :] = jnp.broadcast_to(jnp.sum(mine, axis=1, keepdims=True), (PAIRS, 128))
    hidden = gate.shape[1]
    for k, (first, last) in enumerate(PIECES):
        arrive(k)
        launch(k + 2)
        at = slice(128 * first, 128 * last)
        part = rows[:, at]
        g = jnp.dot(part, gate[at, :], preferred_element_type=F32)
        u = jnp.dot(part, up[at, :], preferred_element_type=F32)
        if k:
            g, u = acc[:, :hidden] + g, acc[:, hidden:] + u
        if k + 1 < len(PIECES):
            lay_out(flat, rows, *PIECES[k + 1])
            acc[:, :hidden] = g
            acc[:, hidden:] = u
    hid[...] = (g / (1.0 + jnp.exp(-g)) * u).astype(BF16)
    for n in range(2):
        arrive(len(PIECES) + n)
        value = jnp.dot(hid[...], down[:, half * n : half * (n + 1)], preferred_element_type=F32)
        for m in range(WIDE // 2):
            part = value[:, lane_tile(m)] * w_ref[...]
            for s in range(SLOTS):
                at = pl.ds(s * WIDE + WIDE // 2 * n + m, PAIRS, stride=PITCH)
                flat[at, :] = part[PAIRS * s : PAIRS * (s + 1)]
    saves = []
    group = PAIRS // 4
    for i in range(4):
        at = slice(group * i, group * (i + 1))
        msg[at] = flat.reshape(PAIRS, PITCH, 128)[at, :MSG, :].astype(BF16)
        saves.append(pltpu.make_async_copy(msg.at[at], out_ref.at[at], sem_out.at[i]))
        saves[-1].start()
    for save in saves:
        save.wait()


def mix_kernel(start, node_ref, local_ref, in_ref, *refs):
    before, (out_ref, flat_ref, rows_ref) = refs[:-3], refs[-3:]
    pick = jnp.concatenate(picks(node_ref, local_ref, start), axis=0).astype(BF16)
    spread(in_ref, flat_ref)
    lay_out(flat_ref, rows_ref, 0, WIDE)
    for k in range(7):
        at = slice(512 * k, 512 * (k + 1))
        value = lax.dot_general(pick, rows_ref[:, at], (((0,), (0,)), ((), ())), preferred_element_type=F32)
        if before:
            value = value + before[0][:, at]
        out_ref[:, at] = value.astype(out_ref.dtype)


def vmem(mib):
    return pltpu.CompilerParams(vmem_limit_bytes=mib << 20)


def body(tokens, node_ids, local_ids, affinity, w_gate, w_up, w_down, grad_parts):
    tok, width = tokens.shape
    hidden = w_gate.shape[2]
    routes = node_ids.T, local_ids.T
    chips, swap = ("edp", "chip"), [(0, 1), (1, 0)]
    core = lax.axis_index("core").astype(I32).reshape(1)
    flat = pltpu.VMEM((PAIRS * PITCH, 128), F32)
    rows = pltpu.VMEM((ROWS, width), BF16)
    anywhere, scalar = pl.BlockSpec(memory_space=pl.ANY), pl.BlockSpec(memory_space=pltpu.SMEM)
    dma = pltpu.SemaphoreType.DMA

    def exchange(message):
        return lax.all_to_all(message, chips, split_axis=0, concat_axis=0, tiled=True)

    def send(start, *grads):
        return pl.pallas_call(
            functools.partial(send_kernel, start),
            out_shape=jax.ShapeDtypeStruct((PAIRS, MSG + (GRAD if grads else 0), 128), BF16),
            scratch_shapes=[flat],
            compiler_params=vmem(32),
            name="send",
        )(*routes, affinity.T, tokens, *grads)

    def experts(message):
        return pl.pallas_call(
            expert_kernel,
            in_specs=[scalar] + [anywhere] * 4,
            out_specs=anywhere,
            out_shape=jax.ShapeDtypeStruct((PAIRS, MSG, 128), BF16),
            scratch_shapes=[
                pltpu.VMEM((PAIRS, MSG, 128), BF16),
                flat,
                rows,
                pltpu.VMEM((width, hidden), BF16),
                pltpu.VMEM((width, hidden), BF16),
                pltpu.VMEM((hidden, width), BF16),
                pltpu.VMEM((ROWS, 2 * hidden), F32),
                pltpu.VMEM((ROWS, hidden), BF16),
                pltpu.VMEM((ROWS, 128), F32),
                dma((1,)),
                dma((len(PIECES),)),
                dma((len(PIECES),)),
                dma((2,)),
                dma((4,)),
            ],
            compiler_params=vmem(50),
            cost_estimate=pl.CostEstimate(
                flops=6 * ROWS * width * hidden, bytes_accessed=6 * width * hidden + 8 * ROWS * width, transcendentals=0
            ),
            name="experts",
        )(core, message, w_gate, w_up, w_down)

    def pair_result(message):
        other = lax.ppermute(message, "core", swap)
        mine = experts(message)
        back = lax.ppermute(experts(other), "core", swap)
        return (mine.astype(F32) + back.astype(F32)).astype(BF16)

    def mix(start, message, *before):
        return pl.pallas_call(
            functools.partial(mix_kernel, start),
            out_shape=jax.ShapeDtypeStruct((tok, width), BF16 if before else F32),
            scratch_shapes=[flat, rows],
            compiler_params=vmem(32),
            name="mix",
        )(*routes, message, *before)

    keep, give = pl.pallas_call(
        halves_kernel,
        in_specs=[scalar, pl.BlockSpec(memory_space=pltpu.VMEM)],
        out_shape=(
            jax.ShapeDtypeStruct((PAIRS, GRAD, 128), F32),
            jax.ShapeDtypeStruct((PAIRS, GRAD, 128), BF16),
        ),
        compiler_params=vmem(32),
        name="halves",
    )(core, grad_parts[0])
    got = lax.ppermute(give, "core", swap)
    arrived = exchange(send(0))
    arrived_2 = exchange(send(SLOTS, keep, got))
    returned = exchange(pair_result(arrived))
    returned_2 = exchange(pair_result(arrived_2))
    mixed = mix(SLOTS, returned_2, mix(0, returned))
    total = jnp.sum(arrived_2[:, MSG:, :].astype(F32), axis=0)
    low = jnp.concatenate([total[:24], total[24:28]], axis=0)
    high = jnp.concatenate([total[28:], total[:24]], axis=0)
    return mixed, jnp.where(core[0] == 0, low, high)


def solution(mesh):
    split = Mesh(mesh.devices.reshape(2, 32, 2), ("edp", "chip", "core"))
    every = ("edp", "chip", "core")
    flat, deep = P(every, None), P(every, None, None)
    return jax.shard_map(
        body,
        mesh=split,
        in_specs=(flat, flat, flat, flat, deep, deep, deep, deep),
        out_specs=(flat, flat),
        check_vma=False,
    )
```

```python
import functools

import jax
import jax.numpy as jnp
from jax import lax
from jax.experimental import pallas as pl
from jax.experimental.pallas import tpu as pltpu
from jax.sharding import Mesh, PartitionSpec as P


PAIRS, SLOTS, WIDE = 64, 5, 28
COEF_AT = SLOTS * WIDE
MSG = COEF_AT + 4
GRAD = 32
PITCH = MSG + 8
ROWS = PAIRS * SLOTS
CUTS = tuple(slice(16 * i, 16 * (i + 1)) for i in range(PAIRS // 16))
F32, BF16, I32 = jnp.float32, jnp.bfloat16, jnp.int32


def iota(shape, dim):
    return lax.broadcasted_iota(I32, shape, dim)


def pair_of(node_ref, local_ref, column):
    return node_ref[column : column + 1, :] * 8 + local_ref[2 * column : 2 * column + 1, :] // 2


def picks(node_ref, local_ref, start):
    tok = node_ref.shape[1]
    pair = iota((PAIRS, tok), 0)
    hit = jnp.zeros((PAIRS, tok), jnp.bool_)
    for column in range(4):
        hit = hit | (pair == pair_of(node_ref, local_ref, column))
    earlier = (iota((tok, tok), 0) < iota((tok, tok), 1)).astype(BF16)
    rank = jnp.dot(hit.astype(F32).astype(BF16), earlier, preferred_element_type=F32)
    return [jnp.where(hit & (rank == float(start + slot)), 1.0, 0.0) for slot in range(SLOTS)]


def lane_tile(j):
    return slice(128 * j, 128 * (j + 1))


def load_all(pairs, sem):
    copies = [pltpu.make_async_copy(src, dst, sem.at[i]) for i, (src, dst) in enumerate(pairs)]
    for copy in copies:
        copy.start()
    return copies


def send_kernel(start, node_in, local_in, aff_in, tok_in, *refs):
    grad_refs, (out_ref, flat_ref, stage_ref, node_ref, local_ref, aff_ref, tok_ref, sem) = refs[:-8], refs[-8:]
    here = ((node_in, node_ref), (local_in, local_ref), (aff_in, aff_ref), (tok_in, tok_ref))
    copies = load_all(here, sem)
    for copy in copies[:3]:
        copy.wait()
    each = picks(node_ref, local_ref, start)
    pick = jnp.concatenate(each, axis=0).astype(BF16)
    copies[3].wait()
    for k in range(7):
        rows = jnp.dot(pick, tok_ref[:, 512 * k : 512 * (k + 1)], preferred_element_type=F32)
        for m in range(4):
            for s in range(SLOTS):
                at = pl.ds(s * WIDE + 4 * k + m, PAIRS, stride=PITCH)
                flat_ref[at, :] = rows[PAIRS * s : PAIRS * (s + 1), lane_tile(m)]
    aff = aff_ref[...]
    weight = 2.5 * aff / jnp.sum(aff, axis=0, keepdims=True)
    tok = node_ref.shape[1]
    pair = iota((PAIRS, tok), 0)
    even = jnp.zeros((PAIRS, tok), F32)
    odd = jnp.zeros((PAIRS, tok), F32)
    for column in range(4):
        first, second = weight[2 * column : 2 * column + 1, :], weight[2 * column + 1 : 2 * column + 2, :]
        flip = local_ref[2 * column : 2 * column + 1, :] % 2 == 1
        here = pair == pair_of(node_ref, local_ref, column)
        even = jnp.where(here, jnp.where(flip, second, first), even)
        odd = jnp.where(here, jnp.where(flip, first, second), odd)
    lane = iota((PAIRS, 128), 1)
    coef = jnp.zeros((PAIRS, 128), F32)
    for slot in range(SLOTS):
        even_w = jnp.sum(each[slot] * even, axis=1, keepdims=True)
        odd_w = jnp.sum(each[slot] * odd, axis=1, keepdims=True)
        coef = jnp.where(lane // 2 == 2 * slot, even_w, coef)
        coef = jnp.where(lane // 2 == 2 * slot + 1, odd_w, coef)
    high = coef.astype(BF16).astype(F32)
    coef = jnp.where(lane % 2 == 0, high, coef - high)
    for row in range(COEF_AT, MSG):
        flat_ref[pl.ds(row, PAIRS, stride=PITCH), :] = coef
    saves = []
    for i, cut in enumerate(CUTS):
        stage_ref[cut, :MSG, :] = flat_ref.reshape(PAIRS, PITCH, 128)[cut, :MSG, :].astype(BF16)
        if grad_refs:
            keep_ref, got_ref = grad_refs
            stage_ref[cut, MSG:, :] = (keep_ref[cut] + got_ref[cut].astype(F32)).astype(BF16)
        saves.append(pltpu.make_async_copy(stage_ref.at[cut], out_ref.at[cut], sem.at[4 + i]))
        saves[-1].start()
    for save in saves:
        save.wait()


def halves_kernel(core_ref, in_ref, keep_ref, give_ref):
    blocks = in_ref.reshape(PAIRS, 2 * WIDE, 128)
    first = core_ref[0] == 0
    low, high = blocks[:, :24, :], blocks[:, 32:, :]
    shared = blocks[:, 24:32, :]
    keep_ref[:, :24, :] = jnp.where(first, low, high)
    keep_ref[:, 24:, :] = shared
    give_ref[:, :24, :] = jnp.where(first, high, low).astype(BF16)
    give_ref[:, 24:, :] = shared.astype(BF16)


def spread(src_ref, flat_ref):
    flat_ref.reshape(PAIRS, PITCH, 128)[:, :MSG, :] = src_ref[:, :MSG, :].astype(F32)


def lay_out(flat_ref, rows_ref, first, last):
    for s in range(SLOTS):
        for j in range(first, last):
            tile = flat_ref[pl.ds(s * WIDE + j, PAIRS, stride=PITCH), :]
            rows_ref[PAIRS * s : PAIRS * (s + 1), lane_tile(j)] = tile.astype(BF16)


PIECE, PIECES = 512, 7


def expert_kernel(
    core_ref, in_ref, gate_ref, up_ref, down_ref, out_ref,
    flat, rows, gate, up, down, acc, hid, w_ref, sem_g, sem_u, sem_d,
):
    hidden = gate.shape[1]

    def cut(k):
        return pl.ds(pl.multiple_of(k * PIECE, PIECE), PIECE)

    def gate_copy(k):
        return pltpu.make_async_copy(gate_ref.at[0, cut(k), :], gate.at[cut(k), :], sem_g.at[k])

    def up_copy(k):
        return pltpu.make_async_copy(up_ref.at[0, cut(k), :], up.at[cut(k), :], sem_u.at[k])

    down_copy = pltpu.make_async_copy(down_ref.at[0], down, sem_d.at[0])
    for k in range(3):
        gate_copy(k).start()
        up_copy(k).start()
    spread(in_ref, flat)
    core = core_ref[0]
    coef = flat[pl.ds(COEF_AT, PAIRS, stride=PITCH), :]
    lane = iota((PAIRS, 128), 1)
    for s in range(SLOTS):
        mine = jnp.where(lane // 2 == 2 * s + core, coef, 0.0)
        w_ref[PAIRS * s : PAIRS * (s + 1), :] = jnp.broadcast_to(jnp.sum(mine, axis=1, keepdims=True), (PAIRS, 128))
    lay_out(flat, rows, 0, WIDE)
    acc[...] = jnp.zeros(acc.shape, F32)

    def piece(k, carry):
        gate_copy(k).wait()
        up_copy(k).wait()

        @pl.when(k + 3 < PIECES)
        def _():
            gate_copy(k + 3).start()
            up_copy(k + 3).start()

        @pl.when(k + 3 == PIECES)
        def _():
            down_copy.start()

        part = rows[:, cut(k)]
        acc[:, :hidden] += jnp.dot(part, gate[cut(k), :], preferred_element_type=F32)
        acc[:, hidden:] += jnp.dot(part, up[cut(k), :], preferred_element_type=F32)
        return carry

    lax.fori_loop(0, PIECES, piece, 0)
    g, u = acc[:, :hidden], acc[:, hidden:]
    hid[...] = (g / (1.0 + jnp.exp(-g)) * u).astype(BF16)
    down_copy.wait()

    def columns(n, carry):
        value = jnp.dot(hid[...], down[:, cut(n)], preferred_element_type=F32)
        for m in range(PIECE // 128):
            part = value[:, lane_tile(m)] * w_ref[...]
            for s in range(SLOTS):
                at = pl.ds(s * WIDE + PIECE // 128 * n + m, PAIRS, stride=PITCH)
                flat[at, :] = part[PAIRS * s : PAIRS * (s + 1)]
        return carry

    lax.fori_loop(0, PIECES, columns, 0)
    out_ref[...] = flat.reshape(PAIRS, PITCH, 128)[:, :MSG, :].astype(BF16)


def mix_kernel(start, node_in, local_in, msg_in, *refs):
    before, (out_ref, flat_ref, rows_ref, node_ref, local_ref, msg_ref, sum_ref, sem) = refs[:-8], refs[-8:]
    here = [(node_in, node_ref), (local_in, local_ref)] + [(msg_in.at[cut], msg_ref.at[cut]) for cut in CUTS]
    copies = load_all(here + [(old, sum_ref) for old in before], sem)
    copies[0].wait()
    copies[1].wait()
    pick = jnp.concatenate(picks(node_ref, local_ref, start), axis=0).astype(BF16)
    for cut, copy in zip(CUTS, copies[2:]):
        copy.wait()
        flat_ref.reshape(PAIRS, PITCH, 128)[cut, :MSG, :] = msg_ref[cut].astype(F32)
    lay_out(flat_ref, rows_ref, 0, WIDE)
    for copy in copies[6:]:
        copy.wait()
    for k in range(7):
        at = slice(512 * k, 512 * (k + 1))
        value = lax.dot_general(pick, rows_ref[:, at], (((0,), (0,)), ((), ())), preferred_element_type=F32)
        if before:
            value = value + sum_ref[:, at]
        out_ref[:, at] = value.astype(out_ref.dtype)


def in_hbm(array):
    return pltpu.with_memory_space_constraint(array, pltpu.HBM)


def vmem(mib):
    return pltpu.CompilerParams(vmem_limit_bytes=mib << 20)


def step(tokens, node_ids, local_ids, affinity, w_gate, w_up, w_down, grad_parts):
    tok, width = tokens.shape
    hidden = w_gate.shape[2]
    routes = node_ids.T, local_ids.T
    chips, swap = ("edp", "chip"), [(0, 1), (1, 0)]
    core = lax.axis_index("core").astype(I32).reshape(1)
    flat = pltpu.VMEM((PAIRS * PITCH, 128), F32)
    rows = pltpu.VMEM((ROWS, width), BF16)
    far, scalar = pl.BlockSpec(memory_space=pltpu.HBM), pl.BlockSpec(memory_space=pltpu.SMEM)
    local = pl.BlockSpec(memory_space=pltpu.VMEM)
    dma = pltpu.SemaphoreType.DMA
    small = [pltpu.VMEM((4, tok), I32), pltpu.VMEM((8, tok), I32)]

    def exchange(message):
        return lax.all_to_all(message, chips, split_axis=0, concat_axis=0, tiled=True)

    def send(start, *grads):
        shape = (PAIRS, MSG + (GRAD if grads else 0), 128)
        return pl.pallas_call(
            functools.partial(send_kernel, start),
            in_specs=[far] * 4 + [local] * len(grads),
            out_specs=far,
            out_shape=pltpu.HBM(shape, BF16),
            scratch_shapes=[flat, pltpu.VMEM(shape, BF16)]
            + small
            + [pltpu.VMEM((8, tok), F32), pltpu.VMEM((tok, width), BF16), dma((8,))],
            compiler_params=vmem(32),
            name="send",
        )(*map(in_hbm, (*routes, affinity.T, tokens)), *grads)

    def experts(message):
        return pl.pallas_call(
            expert_kernel,
            in_specs=[scalar, local] + [far] * 3,
            out_specs=local,
            out_shape=jax.ShapeDtypeStruct((PAIRS, MSG, 128), BF16),
            scratch_shapes=[
                flat,
                rows,
                pltpu.VMEM((width, hidden), BF16),
                pltpu.VMEM((width, hidden), BF16),
                pltpu.VMEM((hidden, width), BF16),
                pltpu.VMEM((ROWS, 2 * hidden), F32),
                pltpu.VMEM((ROWS, hidden), BF16),
                pltpu.VMEM((ROWS, 128), F32),
                dma((PIECES,)),
                dma((PIECES,)),
                dma((1,)),
            ],
            compiler_params=vmem(40),
            cost_estimate=pl.CostEstimate(
                flops=6 * ROWS * width * hidden, bytes_accessed=6 * width * hidden + 8 * ROWS * width, transcendentals=0
            ),
            name="experts",
        )(core, message, *map(in_hbm, (w_gate, w_up, w_down)))

    def pair_result(message):
        other = lax.ppermute(message, "core", swap)
        mine = experts(message)
        theirs = experts(other)
        back = lax.ppermute(theirs, "core", swap)
        return (mine.astype(F32) + back.astype(F32)).astype(BF16)

    def mix(start, message, *before):
        return pl.pallas_call(
            functools.partial(mix_kernel, start),
            in_specs=[far] * (3 + len(before)),
            out_shape=jax.ShapeDtypeStruct((tok, width), BF16) if before else pltpu.HBM((tok, width), F32),
            scratch_shapes=[flat, rows]
            + small
            + [pltpu.VMEM((PAIRS, MSG, 128), BF16), pltpu.VMEM((tok, width), F32), dma((7,))],
            compiler_params=vmem(32),
            name="mix",
        )(*map(in_hbm, (*routes, message, *before)))

    halves = pl.pallas_call(
        halves_kernel,
        in_specs=[scalar, local],
        out_shape=(
            jax.ShapeDtypeStruct((PAIRS, GRAD, 128), F32),
            jax.ShapeDtypeStruct((PAIRS, GRAD, 128), BF16),
        ),
        compiler_params=vmem(32),
        name="halves",
    )
    keep, give = halves(core, grad_parts[0])
    got = lax.ppermute(give, "core", swap)
    message = send(0)
    arrived = exchange(message)
    message_2 = send(SLOTS, keep, got)
    arrived_2 = exchange(message_2)
    result = pair_result(arrived)
    returned = exchange(result)
    result_2 = pair_result(arrived_2)
    returned_2 = exchange(result_2)
    partial = mix(0, returned)
    mixed = mix(SLOTS, returned_2, partial)
    total = jnp.sum(arrived_2[:, MSG:, :].astype(F32), axis=0)
    low = jnp.concatenate([total[:24], total[24:28]], axis=0)
    high = jnp.concatenate([total[28:], total[:24]], axis=0)
    return mixed, jnp.where(core[0] == 0, low, high)


def solution(mesh):
    split = Mesh(mesh.devices.reshape(2, 32, 2), ("edp", "chip", "core"))
    every = ("edp", "chip", "core")
    flat, deep = P(every, None), P(every, None, None)
    return jax.shard_map(
        step,
        mesh=split,
        in_specs=(flat, flat, flat, flat, deep, deep, deep, deep),
        out_specs=(flat, flat),
        check_vma=False,
    )
```

```python
import functools

import jax
import jax.numpy as jnp
from jax import lax
from jax.experimental import pallas as pl
from jax.experimental.pallas import tpu as pltpu
from jax.sharding import Mesh, PartitionSpec as P


PAIRS, SLOTS, WIDE = 64, 5, 28
COEF_AT = SLOTS * WIDE
MSG = COEF_AT + 4
GRAD = 32
PITCH = MSG + 8
ROWS = PAIRS * SLOTS
CUTS = tuple(slice(16 * i, 16 * (i + 1)) for i in range(PAIRS // 16))
F32, BF16, I32 = jnp.float32, jnp.bfloat16, jnp.int32


def iota(shape, dim):
    return lax.broadcasted_iota(I32, shape, dim)


def pair_of(node_ref, local_ref, column):
    return node_ref[column : column + 1, :] * 8 + local_ref[2 * column : 2 * column + 1, :] // 2


def picks(node_ref, local_ref, start):
    tok = node_ref.shape[1]
    pair = iota((PAIRS, tok), 0)
    hit = jnp.zeros((PAIRS, tok), jnp.bool_)
    for column in range(4):
        hit = hit | (pair == pair_of(node_ref, local_ref, column))
    earlier = (iota((tok, tok), 0) < iota((tok, tok), 1)).astype(BF16)
    rank = jnp.dot(hit.astype(F32).astype(BF16), earlier, preferred_element_type=F32)
    return [jnp.where(hit & (rank == float(start + slot)), 1.0, 0.0) for slot in range(SLOTS)]


def lane_tile(j):
    return slice(128 * j, 128 * (j + 1))


def load_all(pairs, sem):
    copies = [pltpu.make_async_copy(src, dst, sem.at[i]) for i, (src, dst) in enumerate(pairs)]
    for copy in copies:
        copy.start()
    return copies


def send_kernel(
    start, node_in, local_in, aff_in, tok_in, out_ref, flat_ref, stage_ref, node_ref, local_ref, aff_ref, tok_ref, sem
):
    here = ((node_in, node_ref), (local_in, local_ref), (aff_in, aff_ref), (tok_in, tok_ref))
    copies = load_all(here, sem)
    for copy in copies[:3]:
        copy.wait()
    each = picks(node_ref, local_ref, start)
    pick = jnp.concatenate(each, axis=0).astype(BF16)
    copies[3].wait()
    for k in range(7):
        rows = jnp.dot(pick, tok_ref[:, 512 * k : 512 * (k + 1)], preferred_element_type=F32)
        for m in range(4):
            for s in range(SLOTS):
                at = pl.ds(s * WIDE + 4 * k + m, PAIRS, stride=PITCH)
                flat_ref[at, :] = rows[PAIRS * s : PAIRS * (s + 1), lane_tile(m)]
    aff = aff_ref[...]
    weight = 2.5 * aff / jnp.sum(aff, axis=0, keepdims=True)
    tok = node_ref.shape[1]
    pair = iota((PAIRS, tok), 0)
    even = jnp.zeros((PAIRS, tok), F32)
    odd = jnp.zeros((PAIRS, tok), F32)
    for column in range(4):
        first, second = weight[2 * column : 2 * column + 1, :], weight[2 * column + 1 : 2 * column + 2, :]
        flip = local_ref[2 * column : 2 * column + 1, :] % 2 == 1
        here = pair == pair_of(node_ref, local_ref, column)
        even = jnp.where(here, jnp.where(flip, second, first), even)
        odd = jnp.where(here, jnp.where(flip, first, second), odd)
    lane = iota((PAIRS, 128), 1)
    coef = jnp.zeros((PAIRS, 128), F32)
    for slot in range(SLOTS):
        even_w = jnp.sum(each[slot] * even, axis=1, keepdims=True)
        odd_w = jnp.sum(each[slot] * odd, axis=1, keepdims=True)
        coef = jnp.where(lane // 2 == 2 * slot, even_w, coef)
        coef = jnp.where(lane // 2 == 2 * slot + 1, odd_w, coef)
    high = coef.astype(BF16).astype(F32)
    coef = jnp.where(lane % 2 == 0, high, coef - high)
    for row in range(COEF_AT, MSG):
        flat_ref[pl.ds(row, PAIRS, stride=PITCH), :] = coef
    saves = []
    for i, cut in enumerate(CUTS):
        stage_ref[cut] = flat_ref.reshape(PAIRS, PITCH, 128)[cut, :MSG, :].astype(BF16)
        saves.append(pltpu.make_async_copy(stage_ref.at[cut], out_ref.at[cut], sem.at[4 + i]))
        saves[-1].start()
    for save in saves:
        save.wait()


def halves_kernel(core_ref, in_ref, keep_ref, give_ref):
    blocks = in_ref.reshape(PAIRS, 2 * WIDE, 128)
    first = core_ref[0] == 0
    low, high = blocks[:, :24, :], blocks[:, 32:, :]
    shared = blocks[:, 24:32, :]
    keep_ref[:, :24, :] = jnp.where(first, low, high)
    keep_ref[:, 24:, :] = shared
    give_ref[:, :24, :] = jnp.where(first, high, low).astype(BF16)
    give_ref[:, 24:, :] = shared.astype(BF16)


def spread(src_ref, flat_ref):
    flat_ref.reshape(PAIRS, PITCH, 128)[:, :MSG, :] = src_ref[:, :MSG, :].astype(F32)


def lay_out(flat_ref, rows_ref, first, last):
    for s in range(SLOTS):
        for j in range(first, last):
            tile = flat_ref[pl.ds(s * WIDE + j, PAIRS, stride=PITCH), :]
            rows_ref[PAIRS * s : PAIRS * (s + 1), lane_tile(j)] = tile.astype(BF16)


PIECE, PIECES, DEPTH = 512, 7, 4


def expert_kernel(
    core_ref, own_ref, other_ref, gate_ref, up_ref, down_ref, mine_ref, theirs_ref,
    flats, rows, gate, up, down, acc, hid, w_ref, sem_g, sem_u, sem_d,
):
    hidden = gate.shape[2]

    def cut(k):
        return pl.ds(pl.multiple_of(k * PIECE, PIECE), PIECE)

    def gate_copy(k):
        slot = lax.rem(k, DEPTH)
        return pltpu.make_async_copy(gate_ref.at[0, cut(k), :], gate.at[slot], sem_g.at[slot])

    def up_copy(k):
        slot = lax.rem(k, DEPTH)
        return pltpu.make_async_copy(up_ref.at[0, cut(k), :], up.at[slot], sem_u.at[slot])

    down_copy = pltpu.make_async_copy(down_ref.at[0], down, sem_d.at[0])
    for k in range(DEPTH - 1):
        gate_copy(k).start()
        up_copy(k).start()
    core = core_ref[0]
    lane = iota((PAIRS, 128), 1)
    for side, in_ref in enumerate((own_ref, other_ref)):
        flat = flats.at[side]
        spread(in_ref, flat)
        coef = flat[pl.ds(COEF_AT, PAIRS, stride=PITCH), :]
        for s in range(SLOTS):
            mine = jnp.where(lane // 2 == 2 * s + core, coef, 0.0)
            at = ROWS * side + PAIRS * s
            w_ref[at : at + PAIRS, :] = jnp.broadcast_to(jnp.sum(mine, axis=1, keepdims=True), (PAIRS, 128))
        lay_out(flat, rows.at[ROWS * side : ROWS * (side + 1)], 0, WIDE)
    acc[...] = jnp.zeros(acc.shape, F32)

    def piece(k, carry):
        slot = lax.rem(k, DEPTH)
        gate_copy(k).wait()
        up_copy(k).wait()

        @pl.when(k + DEPTH - 1 < PIECES)
        def _():
            gate_copy(k + DEPTH - 1).start()
            up_copy(k + DEPTH - 1).start()

        @pl.when(k + DEPTH - 1 == PIECES)
        def _():
            down_copy.start()

        part = rows[:, cut(k)]
        acc[:, :hidden] += jnp.dot(part, gate[slot], preferred_element_type=F32)
        acc[:, hidden:] += jnp.dot(part, up[slot], preferred_element_type=F32)
        return carry

    lax.fori_loop(0, PIECES, piece, 0)
    g, u = acc[:, :hidden], acc[:, hidden:]
    hid[...] = (g / (1.0 + jnp.exp(-g)) * u).astype(BF16)
    down_copy.wait()

    def columns(n, carry):
        value = jnp.dot(hid[...], down[:, cut(n)], preferred_element_type=F32)
        for m in range(PIECE // 128):
            part = value[:, lane_tile(m)] * w_ref[...]
            for s in range(2 * SLOTS):
                at = pl.ds(s % SLOTS * WIDE + PIECE // 128 * n + m, PAIRS, stride=PITCH)
                flats[s // SLOTS, at, :] = part[PAIRS * s : PAIRS * (s + 1)]
        return carry

    lax.fori_loop(0, PIECES, columns, 0)
    for side, out_ref in enumerate((mine_ref, theirs_ref)):
        out_ref[...] = flats.at[side].reshape(PAIRS, PITCH, 128)[:, :MSG, :].astype(BF16)


def fold_kernel(place_ref, *refs):
    parts, (total_ref, outs) = refs[:-5], (refs[-1], refs[-5:-1])
    total = parts[0][...].astype(F32)
    for part in parts[1:]:
        total = total + part[...].astype(F32)
    total_ref[...] = total
    size = total_ref.shape[0] // 4
    for flip, out_ref in enumerate(outs):
        at = jnp.bitwise_xor(place_ref[0], flip) * size
        out_ref[...] = total_ref[pl.ds(at, size)].astype(out_ref.dtype)


def mix_kernel(start, node_in, local_in, in_ref, *refs):
    before, (out_ref, flat_ref, rows_ref, node_ref, local_ref, sum_ref, sem) = refs[:-7], refs[-7:]
    copies = load_all([(node_in, node_ref), (local_in, local_ref)] + [(old, sum_ref) for old in before], sem)
    copies[0].wait()
    copies[1].wait()
    pick = jnp.concatenate(picks(node_ref, local_ref, start), axis=0).astype(BF16)
    spread(in_ref, flat_ref)
    lay_out(flat_ref, rows_ref, 0, WIDE)
    for copy in copies[2:]:
        copy.wait()
    for k in range(7):
        at = slice(512 * k, 512 * (k + 1))
        value = lax.dot_general(pick, rows_ref[:, at], (((0,), (0,)), ((), ())), preferred_element_type=F32)
        if before:
            value = value + sum_ref[:, at]
        out_ref[:, at] = value.astype(out_ref.dtype)


def in_hbm(array):
    return pltpu.with_memory_space_constraint(array, pltpu.HBM)


def place(axes):
    return lax.axis_index(axes).astype(I32).reshape(1)


def vmem(mib):
    return pltpu.CompilerParams(vmem_limit_bytes=mib << 20)


def step(tokens, node_ids, local_ids, affinity, w_gate, w_up, w_down, grad_parts):
    tok, width = tokens.shape
    hidden = w_gate.shape[2]
    routes = node_ids.T, local_ids.T
    chips, swap = ("edp", "zh", "x", "y"), [(0, 1), (1, 0)]
    core = place("core")
    flat = pltpu.VMEM((PAIRS * PITCH, 128), F32)
    rows = pltpu.VMEM((ROWS, width), BF16)
    far, scalar = pl.BlockSpec(memory_space=pltpu.HBM), pl.BlockSpec(memory_space=pltpu.SMEM)
    local = pl.BlockSpec(memory_space=pltpu.VMEM)
    dma = pltpu.SemaphoreType.DMA
    small = [pltpu.VMEM((4, tok), I32), pltpu.VMEM((8, tok), I32)]

    def exchange(message):
        return lax.all_to_all(message, chips, split_axis=0, concat_axis=0, tiled=True)

    def send(start):
        shape = (PAIRS, MSG, 128)
        return pl.pallas_call(
            functools.partial(send_kernel, start),
            in_specs=[far] * 4,
            out_specs=far,
            out_shape=pltpu.HBM(shape, BF16),
            scratch_shapes=[flat, pltpu.VMEM(shape, BF16)]
            + small
            + [pltpu.VMEM((8, tok), F32), pltpu.VMEM((tok, width), BF16), dma((8,))],
            compiler_params=vmem(32),
            name="send",
        )(*map(in_hbm, (*routes, affinity.T, tokens)))

    def experts(own, other):
        shape = jax.ShapeDtypeStruct((PAIRS, MSG, 128), BF16)
        return pl.pallas_call(
            expert_kernel,
            in_specs=[scalar, local, local] + [far] * 3,
            out_specs=(local, local),
            out_shape=(shape, shape),
            scratch_shapes=[
                pltpu.VMEM((2, PAIRS * PITCH, 128), F32),
                pltpu.VMEM((2 * ROWS, width), BF16),
                pltpu.VMEM((DEPTH, PIECE, hidden), BF16),
                pltpu.VMEM((DEPTH, PIECE, hidden), BF16),
                pltpu.VMEM((hidden, width), BF16),
                pltpu.VMEM((2 * ROWS, 2 * hidden), F32),
                pltpu.VMEM((2 * ROWS, hidden), BF16),
                pltpu.VMEM((2 * ROWS, 128), F32),
                dma((DEPTH,)),
                dma((DEPTH,)),
                dma((1,)),
            ],
            compiler_params=vmem(46),
            cost_estimate=pl.CostEstimate(
                flops=12 * ROWS * width * hidden, bytes_accessed=6 * width * hidden + 16 * ROWS * width, transcendentals=0
            ),
            name="experts",
        )(core, own, other, *map(in_hbm, (w_gate, w_up, w_down)))

    def pair_result(message):
        other = lax.ppermute(message, "core", swap)
        mine, theirs = experts(message, other)
        back = lax.ppermute(theirs, "core", swap)
        return (mine.astype(F32) + back.astype(F32)).astype(BF16)

    def fold(axes, dtype, *parts):
        size = parts[0].shape[0] // 4
        shapes = [jax.ShapeDtypeStruct((size, GRAD, 128), F32)] + [jax.ShapeDtypeStruct((size, GRAD, 128), dtype)] * 3
        kept, *given = pl.pallas_call(
            fold_kernel,
            in_specs=[scalar] + [local] * len(parts),
            out_specs=[local] * 4,
            out_shape=shapes,
            scratch_shapes=[pltpu.VMEM(parts[0].shape, F32)],
            compiler_params=vmem(16),
            name="fold",
        )(place(axes), *parts)
        return [kept] + [
            lax.ppermute(part, axes, [(i, i ^ flip) for i in range(4)]) for flip, part in enumerate(given, 1)
        ]

    def mix(start, message, *before):
        return pl.pallas_call(
            functools.partial(mix_kernel, start),
            in_specs=[far, far, local] + [far] * len(before),
            out_shape=jax.ShapeDtypeStruct((tok, width), BF16) if before else pltpu.HBM((tok, width), F32),
            scratch_shapes=[flat, rows]
            + small
            + [pltpu.VMEM((tok, width), F32), dma((3,))],
            compiler_params=vmem(32),
            name="mix",
        )(*map(in_hbm, routes), message, *map(in_hbm, before))

    halves = pl.pallas_call(
        halves_kernel,
        in_specs=[scalar, local],
        out_shape=(
            jax.ShapeDtypeStruct((PAIRS, GRAD, 128), F32),
            jax.ShapeDtypeStruct((PAIRS, GRAD, 128), BF16),
        ),
        compiler_params=vmem(32),
        name="halves",
    )
    keep, give = halves(core, grad_parts[0])
    got = lax.ppermute(give, "core", swap)
    parts = fold(("edp", "zh"), BF16, keep, got)
    parts = fold("x", F32, *parts)
    parts = fold("y", F32, *parts)
    total = (parts[0] + parts[1] + parts[2] + parts[3])[0]
    low = total[:WIDE]
    high = jnp.concatenate([total[WIDE:], total[:24]], axis=0)
    router_grad = jnp.where(core[0] == 0, low, high)
    message = send(0)
    arrived = exchange(message)
    message_2 = send(SLOTS)
    arrived_2 = exchange(message_2)
    result = pair_result(arrived)
    returned = exchange(result)
    result_2 = pair_result(arrived_2)
    returned_2 = exchange(result_2)
    partial = mix(0, returned)
    return mix(SLOTS, returned_2, partial), router_grad


def solution(mesh):
    axes = ("edp", "zh", "x", "y", "core")
    split = Mesh(mesh.devices.reshape(2, 2, 4, 4, 2), axes)
    flat, deep = P(axes, None), P(axes, None, None)
    return jax.shard_map(
        step,
        mesh=split,
        in_specs=(flat, flat, flat, flat, deep, deep, deep, deep),
        out_specs=(flat, flat),
        check_vma=False,
    )
```

```python
import functools

import jax
import jax.numpy as jnp
from jax import lax
from jax.experimental import pallas as pl
from jax.experimental.pallas import tpu as pltpu
from jax.sharding import Mesh, PartitionSpec as P


PAIRS, SLOTS, WIDE = 64, 5, 28
COEF_AT = SLOTS * WIDE
MSG = COEF_AT + 4
GRAD = 32
PITCH = MSG + 8
ROWS = PAIRS * SLOTS
CUTS = tuple(slice(16 * i, 16 * (i + 1)) for i in range(PAIRS // 16))
F32, BF16, I32 = jnp.float32, jnp.bfloat16, jnp.int32


def iota(shape, dim):
    return lax.broadcasted_iota(I32, shape, dim)


def pair_of(node_ref, local_ref, column):
    return node_ref[column : column + 1, :] * 8 + local_ref[2 * column : 2 * column + 1, :] // 2


def picks(node_ref, local_ref, start):
    tok = node_ref.shape[1]
    pair = iota((PAIRS, tok), 0)
    hit = jnp.zeros((PAIRS, tok), jnp.bool_)
    for column in range(4):
        hit = hit | (pair == pair_of(node_ref, local_ref, column))
    earlier = (iota((tok, tok), 0) < iota((tok, tok), 1)).astype(BF16)
    rank = jnp.dot(hit.astype(F32).astype(BF16), earlier, preferred_element_type=F32)
    return [jnp.where(hit & (rank == float(start + slot)), 1.0, 0.0) for slot in range(SLOTS)]


def lane_tile(j):
    return slice(128 * j, 128 * (j + 1))


def load_all(pairs, sem):
    copies = [pltpu.make_async_copy(src, dst, sem.at[i]) for i, (src, dst) in enumerate(pairs)]
    for copy in copies:
        copy.start()
    return copies


def send_kernel(
    start, node_in, local_in, aff_in, tok_in, out_ref, flat_ref, stage_ref, node_ref, local_ref, aff_ref, tok_ref, sem
):
    here = ((node_in, node_ref), (local_in, local_ref), (aff_in, aff_ref), (tok_in, tok_ref))
    copies = load_all(here, sem)
    for copy in copies[:3]:
        copy.wait()
    each = picks(node_ref, local_ref, start)
    pick = jnp.concatenate(each, axis=0).astype(BF16)
    copies[3].wait()
    for k in range(7):
        rows = jnp.dot(pick, tok_ref[:, 512 * k : 512 * (k + 1)], preferred_element_type=F32)
        for m in range(4):
            for s in range(SLOTS):
                at = pl.ds(s * WIDE + 4 * k + m, PAIRS, stride=PITCH)
                flat_ref[at, :] = rows[PAIRS * s : PAIRS * (s + 1), lane_tile(m)]
    aff = aff_ref[...]
    weight = 2.5 * aff / jnp.sum(aff, axis=0, keepdims=True)
    tok = node_ref.shape[1]
    pair = iota((PAIRS, tok), 0)
    even = jnp.zeros((PAIRS, tok), F32)
    odd = jnp.zeros((PAIRS, tok), F32)
    for column in range(4):
        first, second = weight[2 * column : 2 * column + 1, :], weight[2 * column + 1 : 2 * column + 2, :]
        flip = local_ref[2 * column : 2 * column + 1, :] % 2 == 1
        here = pair == pair_of(node_ref, local_ref, column)
        even = jnp.where(here, jnp.where(flip, second, first), even)
        odd = jnp.where(here, jnp.where(flip, first, second), odd)
    lane = iota((PAIRS, 128), 1)
    coef = jnp.zeros((PAIRS, 128), F32)
    for slot in range(SLOTS):
        even_w = jnp.sum(each[slot] * even, axis=1, keepdims=True)
        odd_w = jnp.sum(each[slot] * odd, axis=1, keepdims=True)
        coef = jnp.where(lane // 2 == 2 * slot, even_w, coef)
        coef = jnp.where(lane // 2 == 2 * slot + 1, odd_w, coef)
    high = coef.astype(BF16).astype(F32)
    coef = jnp.where(lane % 2 == 0, high, coef - high)
    for row in range(COEF_AT, MSG):
        flat_ref[pl.ds(row, PAIRS, stride=PITCH), :] = coef
    saves = []
    for i, cut in enumerate(CUTS):
        stage_ref[cut] = flat_ref.reshape(PAIRS, PITCH, 128)[cut, :MSG, :].astype(BF16)
        saves.append(pltpu.make_async_copy(stage_ref.at[cut], out_ref.at[cut], sem.at[4 + i]))
        saves[-1].start()
    for save in saves:
        save.wait()


def halves_kernel(core_ref, in_ref, keep_ref, give_ref):
    blocks = in_ref.reshape(PAIRS, 2 * WIDE, 128)
    first = core_ref[0] == 0
    low, high = blocks[:, :24, :], blocks[:, 32:, :]
    shared = blocks[:, 24:32, :]
    keep_ref[:, :24, :] = jnp.where(first, low, high)
    keep_ref[:, 24:, :] = shared
    give_ref[:, :24, :] = jnp.where(first, high, low).astype(BF16)
    give_ref[:, 24:, :] = shared.astype(BF16)


def spread(src_ref, flat_ref):
    flat_ref.reshape(PAIRS, PITCH, 128)[:, :MSG, :] = src_ref[:, :MSG, :].astype(F32)


def lay_out(flat_ref, rows_ref, first, last):
    for s in range(SLOTS):
        for j in range(first, last):
            tile = flat_ref[pl.ds(s * WIDE + j, PAIRS, stride=PITCH), :]
            rows_ref[PAIRS * s : PAIRS * (s + 1), lane_tile(j)] = tile.astype(BF16)


PIECE, PIECES, BLOCK = 1792, 2, 512


def expert_kernel(
    core_ref, own_ref, other_ref, gate_ref, up_ref, down_ref, mine_ref, theirs_ref,
    flat, rows, gate, up, down, acc, hid, w_ref, sem_g, sem_u, sem_d,
):
    hidden = gate.shape[2]

    def copies(k):
        at = pl.ds(pl.multiple_of(k * PIECE, PIECE), PIECE)
        return (
            pltpu.make_async_copy(gate_ref.at[0, at, :], gate.at[k], sem_g.at[k]),
            pltpu.make_async_copy(up_ref.at[0, at, :], up.at[k], sem_u.at[k]),
        )

    for k in range(PIECES):
        for copy in copies(k):
            copy.start()
    down_copy = pltpu.make_async_copy(down_ref.at[0], down, sem_d.at[0])
    down_copy.start()
    core = core_ref[0]
    lane = iota((PAIRS, 128), 1)
    for side, in_ref in enumerate((own_ref, other_ref)):
        spread(in_ref, flat)
        coef = flat[pl.ds(COEF_AT, PAIRS, stride=PITCH), :]
        for s in range(SLOTS):
            mine = jnp.where(lane // 2 == 2 * s + core, coef, 0.0)
            at = ROWS * side + PAIRS * s
            w_ref[at : at + PAIRS, :] = jnp.broadcast_to(jnp.sum(mine, axis=1, keepdims=True), (PAIRS, 128))
        for s in range(SLOTS):
            at = ROWS * side + PAIRS * s
            for j in range(WIDE):
                tile = flat[pl.ds(s * WIDE + j, PAIRS, stride=PITCH), :]
                half = WIDE // PIECES
                rows[j // half, at : at + PAIRS, lane_tile(j % half)] = tile.astype(BF16)
    acc[...] = jnp.zeros(acc.shape, F32)

    def piece(k, carry):
        for copy in copies(k):
            copy.wait()
        acc[:, :hidden] += jnp.dot(rows[k], gate[k], preferred_element_type=F32)
        acc[:, hidden:] += jnp.dot(rows[k], up[k], preferred_element_type=F32)
        return carry

    lax.fori_loop(0, PIECES, piece, 0)
    for n in range(0, hidden, 256):
        g, u = acc[:, n : n + 256], acc[:, hidden + n : hidden + n + 256]
        hid[:, n : n + 256] = (g / (1.0 + jnp.exp(-g)) * u).astype(BF16)
    down_copy.wait()
    for side, out_ref in enumerate((mine_ref, theirs_ref)):
        here = slice(ROWS * side, ROWS * (side + 1))

        def columns(n, carry):
            at = pl.ds(pl.multiple_of(n * BLOCK, BLOCK), BLOCK)
            value = jnp.dot(hid[here, :], down[:, at], preferred_element_type=F32)
            for m in range(BLOCK // 128):
                part = value[:, lane_tile(m)] * w_ref[here, :]
                for s in range(SLOTS):
                    to = pl.ds(s * WIDE + BLOCK // 128 * n + m, PAIRS, stride=PITCH)
                    flat[to, :] = part[PAIRS * s : PAIRS * (s + 1)]
            return carry

        lax.fori_loop(0, down.shape[1] // BLOCK, columns, 0)
        out_ref[...] = flat.reshape(PAIRS, PITCH, 128)[:, :MSG, :].astype(BF16)


def expert_call(width, hidden):
    scalar, local = pl.BlockSpec(memory_space=pltpu.SMEM), pl.BlockSpec(memory_space=pltpu.VMEM)
    far, dma = pl.BlockSpec(memory_space=pltpu.HBM), pltpu.SemaphoreType.DMA
    shape = jax.ShapeDtypeStruct((PAIRS, MSG, 128), BF16)
    return pl.pallas_call(
        expert_kernel,
        in_specs=[scalar, local, local] + [far] * 3,
        out_specs=(local, local),
        out_shape=(shape, shape),
        scratch_shapes=[
            pltpu.VMEM((PAIRS * PITCH, 128), F32),
            pltpu.VMEM((PIECES, 2 * ROWS, PIECE), BF16),
            pltpu.VMEM((PIECES, PIECE, hidden), BF16),
            pltpu.VMEM((PIECES, PIECE, hidden), BF16),
            pltpu.VMEM((hidden, width), BF16),
            pltpu.VMEM((2 * ROWS, 2 * hidden), F32),
            pltpu.VMEM((2 * ROWS, hidden), BF16),
            pltpu.VMEM((2 * ROWS, 128), F32),
            dma((PIECES,)),
            dma((PIECES,)),
            dma((1,)),
        ],
        compiler_params=vmem(44),
        cost_estimate=pl.CostEstimate(
            flops=12 * ROWS * width * hidden, bytes_accessed=6 * width * hidden + 16 * ROWS * width, transcendentals=0
        ),
        name="experts",
    )


def fold_kernel(place_ref, *refs):
    parts, (total_ref, outs) = refs[:-5], (refs[-1], refs[-5:-1])
    total = parts[0][...].astype(F32)
    for part in parts[1:]:
        total = total + part[...].astype(F32)
    total_ref[...] = total
    size = total_ref.shape[0] // 4
    for flip, out_ref in enumerate(outs):
        at = jnp.bitwise_xor(place_ref[0], flip) * size
        out_ref[...] = total_ref[pl.ds(at, size)].astype(out_ref.dtype)


def mix_kernel(start, node_in, local_in, in_ref, *refs):
    before, (out_ref, flat_ref, rows_ref, node_ref, local_ref, sum_ref, sem) = refs[:-7], refs[-7:]
    copies = load_all([(node_in, node_ref), (local_in, local_ref)] + [(old, sum_ref) for old in before], sem)
    copies[0].wait()
    copies[1].wait()
    pick = jnp.concatenate(picks(node_ref, local_ref, start), axis=0).astype(BF16)
    spread(in_ref, flat_ref)
    lay_out(flat_ref, rows_ref, 0, WIDE)
    for copy in copies[2:]:
        copy.wait()
    for k in range(7):
        at = slice(512 * k, 512 * (k + 1))
        value = lax.dot_general(pick, rows_ref[:, at], (((0,), (0,)), ((), ())), preferred_element_type=F32)
        if before:
            value = value + sum_ref[:, at]
        out_ref[:, at] = value.astype(out_ref.dtype)


def in_hbm(array):
    return pltpu.with_memory_space_constraint(array, pltpu.HBM)


def place(axes):
    return lax.axis_index(axes).astype(I32).reshape(1)


def vmem(mib):
    return pltpu.CompilerParams(vmem_limit_bytes=mib << 20)


def step(tokens, node_ids, local_ids, affinity, w_gate, w_up, w_down, grad_parts):
    tok, width = tokens.shape
    hidden = w_gate.shape[2]
    routes = node_ids.T, local_ids.T
    chips, swap = ("edp", "zh", "x", "y"), [(0, 1), (1, 0)]
    core = place("core")
    flat = pltpu.VMEM((PAIRS * PITCH, 128), F32)
    rows = pltpu.VMEM((ROWS, width), BF16)
    far, scalar = pl.BlockSpec(memory_space=pltpu.HBM), pl.BlockSpec(memory_space=pltpu.SMEM)
    local = pl.BlockSpec(memory_space=pltpu.VMEM)
    dma = pltpu.SemaphoreType.DMA
    small = [pltpu.VMEM((4, tok), I32), pltpu.VMEM((8, tok), I32)]

    def exchange(message):
        return lax.all_to_all(message, chips, split_axis=0, concat_axis=0, tiled=True)

    def send(start):
        shape = (PAIRS, MSG, 128)
        return pl.pallas_call(
            functools.partial(send_kernel, start),
            in_specs=[far] * 4,
            out_specs=far,
            out_shape=pltpu.HBM(shape, BF16),
            scratch_shapes=[flat, pltpu.VMEM(shape, BF16)]
            + small
            + [pltpu.VMEM((8, tok), F32), pltpu.VMEM((tok, width), BF16), dma((8,))],
            compiler_params=vmem(32),
            name="send",
        )(*map(in_hbm, (*routes, affinity.T, tokens)))

    def experts(own, other):
        return expert_call(width, hidden)(core, own, other, *map(in_hbm, (w_gate, w_up, w_down)))

    def pair_result(message):
        other = lax.ppermute(message, "core", swap)
        mine, theirs = experts(message, other)
        back = lax.ppermute(theirs, "core", swap)
        return (mine.astype(F32) + back.astype(F32)).astype(BF16)

    def fold(axes, dtype, *parts):
        size = parts[0].shape[0] // 4
        shapes = [jax.ShapeDtypeStruct((size, GRAD, 128), F32)] + [jax.ShapeDtypeStruct((size, GRAD, 128), dtype)] * 3
        kept, *given = pl.pallas_call(
            fold_kernel,
            in_specs=[scalar] + [local] * len(parts),
            out_specs=[local] * 4,
            out_shape=shapes,
            scratch_shapes=[pltpu.VMEM(parts[0].shape, F32)],
            compiler_params=vmem(16),
            name="fold",
        )(place(axes), *parts)
        return [kept] + [
            lax.ppermute(part, axes, [(i, i ^ flip) for i in range(4)]) for flip, part in enumerate(given, 1)
        ]

    def mix(start, message, *before):
        return pl.pallas_call(
            functools.partial(mix_kernel, start),
            in_specs=[far, far, local] + [far] * len(before),
            out_shape=jax.ShapeDtypeStruct((tok, width), BF16) if before else pltpu.HBM((tok, width), F32),
            scratch_shapes=[flat, rows]
            + small
            + [pltpu.VMEM((tok, width), F32), dma((3,))],
            compiler_params=vmem(32),
            name="mix",
        )(*map(in_hbm, routes), message, *map(in_hbm, before))

    halves = pl.pallas_call(
        halves_kernel,
        in_specs=[scalar, local],
        out_shape=(
            jax.ShapeDtypeStruct((PAIRS, GRAD, 128), F32),
            jax.ShapeDtypeStruct((PAIRS, GRAD, 128), BF16),
        ),
        compiler_params=vmem(32),
        name="halves",
    )
    keep, give = halves(core, grad_parts[0])
    got = lax.ppermute(give, "core", swap)
    parts = fold(("edp", "zh"), BF16, keep, got)
    parts = fold("x", F32, *parts)
    parts = fold("y", F32, *parts)
    total = (parts[0] + parts[1] + parts[2] + parts[3])[0]
    low = total[:WIDE]
    high = jnp.concatenate([total[WIDE:], total[:24]], axis=0)
    router_grad = jnp.where(core[0] == 0, low, high)
    message = send(0)
    arrived = exchange(message)
    message_2 = send(SLOTS)
    arrived_2 = exchange(message_2)
    result = pair_result(arrived)
    returned = exchange(result)
    result_2 = pair_result(arrived_2)
    returned_2 = exchange(result_2)
    partial = mix(0, returned)
    return mix(SLOTS, returned_2, partial), router_grad


def solution(mesh):
    axes = ("edp", "zh", "x", "y", "core")
    split = Mesh(mesh.devices.reshape(2, 2, 4, 4, 2), axes)
    flat, deep = P(axes, None), P(axes, None, None)
    return jax.shard_map(
        step,
        mesh=split,
        in_specs=(flat, flat, flat, flat, deep, deep, deep, deep),
        out_specs=(flat, flat),
        check_vma=False,
    )
```

```python
import functools

import jax
import jax.numpy as jnp
from jax import lax
from jax.experimental import pallas as pl
from jax.experimental.pallas import tpu as pltpu
from jax.sharding import Mesh, PartitionSpec as P


PAIRS, SLOTS, WIDE = 64, 5, 28
COEF_AT = SLOTS * WIDE
MSG = COEF_AT + 4
GRAD = 32
PITCH = MSG + 8
ROWS = PAIRS * SLOTS
CUTS = tuple(slice(16 * i, 16 * (i + 1)) for i in range(PAIRS // 16))
F32, BF16, I32 = jnp.float32, jnp.bfloat16, jnp.int32


def iota(shape, dim):
    return lax.broadcasted_iota(I32, shape, dim)


def pair_of(node_ref, local_ref, column):
    return node_ref[column : column + 1, :] * 8 + local_ref[2 * column : 2 * column + 1, :] // 2


def picks(node_ref, local_ref, start):
    tok = node_ref.shape[1]
    pair = iota((PAIRS, tok), 0)
    hit = jnp.zeros((PAIRS, tok), jnp.bool_)
    for column in range(4):
        hit = hit | (pair == pair_of(node_ref, local_ref, column))
    earlier = (iota((tok, tok), 0) < iota((tok, tok), 1)).astype(BF16)
    rank = jnp.dot(hit.astype(F32).astype(BF16), earlier, preferred_element_type=F32)
    return [jnp.where(hit & (rank == float(start + slot)), 1.0, 0.0) for slot in range(SLOTS)]


def lane_tile(j):
    return slice(128 * j, 128 * (j + 1))


def load_all(pairs, sem):
    copies = [pltpu.make_async_copy(src, dst, sem.at[i]) for i, (src, dst) in enumerate(pairs)]
    for copy in copies:
        copy.start()
    return copies


def send_kernel(
    start, node_in, local_in, aff_in, tok_in, out_ref, flat_ref, stage_ref, node_ref, local_ref, aff_ref, tok_ref, sem
):
    here = ((node_in, node_ref), (local_in, local_ref), (aff_in, aff_ref), (tok_in, tok_ref))
    copies = load_all(here, sem)
    for copy in copies[:3]:
        copy.wait()
    each = picks(node_ref, local_ref, start)
    pick = jnp.concatenate(each, axis=0).astype(BF16)
    copies[3].wait()
    for k in range(7):
        rows = jnp.dot(pick, tok_ref[:, 512 * k : 512 * (k + 1)], preferred_element_type=F32)
        for m in range(4):
            for s in range(SLOTS):
                at = pl.ds(s * WIDE + 4 * k + m, PAIRS, stride=PITCH)
                flat_ref[at, :] = rows[PAIRS * s : PAIRS * (s + 1), lane_tile(m)]
    aff = aff_ref[...]
    weight = 2.5 * aff / jnp.sum(aff, axis=0, keepdims=True)
    tok = node_ref.shape[1]
    pair = iota((PAIRS, tok), 0)
    even = jnp.zeros((PAIRS, tok), F32)
    odd = jnp.zeros((PAIRS, tok), F32)
    for column in range(4):
        first, second = weight[2 * column : 2 * column + 1, :], weight[2 * column + 1 : 2 * column + 2, :]
        flip = local_ref[2 * column : 2 * column + 1, :] % 2 == 1
        here = pair == pair_of(node_ref, local_ref, column)
        even = jnp.where(here, jnp.where(flip, second, first), even)
        odd = jnp.where(here, jnp.where(flip, first, second), odd)
    lane = iota((PAIRS, 128), 1)
    coef = jnp.zeros((PAIRS, 128), F32)
    for slot in range(SLOTS):
        even_w = jnp.sum(each[slot] * even, axis=1, keepdims=True)
        odd_w = jnp.sum(each[slot] * odd, axis=1, keepdims=True)
        coef = jnp.where(lane // 2 == 2 * slot, even_w, coef)
        coef = jnp.where(lane // 2 == 2 * slot + 1, odd_w, coef)
    high = coef.astype(BF16).astype(F32)
    coef = jnp.where(lane % 2 == 0, high, coef - high)
    for row in range(COEF_AT, MSG):
        flat_ref[pl.ds(row, PAIRS, stride=PITCH), :] = coef
    saves = []
    for i, cut in enumerate(CUTS):
        stage_ref[cut] = flat_ref.reshape(PAIRS, PITCH, 128)[cut, :MSG, :].astype(BF16)
        saves.append(pltpu.make_async_copy(stage_ref.at[cut], out_ref.at[cut], sem.at[4 + i]))
        saves[-1].start()
    for save in saves:
        save.wait()


def halves_kernel(core_ref, in_ref, keep_ref, give_ref):
    blocks = in_ref.reshape(PAIRS, 2 * WIDE, 128)
    first = core_ref[0] == 0
    low, high = blocks[:, :24, :], blocks[:, 32:, :]
    shared = blocks[:, 24:32, :]
    keep_ref[:, :24, :] = jnp.where(first, low, high)
    keep_ref[:, 24:, :] = shared
    give_ref[:, :24, :] = jnp.where(first, high, low).astype(BF16)
    give_ref[:, 24:, :] = shared.astype(BF16)


def lay_out(flat_ref, rows_ref, first, last):
    for s in range(SLOTS):
        for j in range(first, last):
            tile = flat_ref[pl.ds(s * WIDE + j, PAIRS, stride=PITCH), :]
            rows_ref[PAIRS * s : PAIRS * (s + 1), lane_tile(j)] = tile.astype(BF16)


PIECE, PIECES, DEPTH = 512, 7, 4


def expert_kernel(
    core_ref, own_ref, other_ref, gate_ref, up_ref, down_ref, mine_ref, theirs_ref,
    msgs, sem_m, flats, rows, gate, up, down, acc, hid, w_ref, sem_g, sem_u, sem_d,
):
    hidden = gate.shape[2]

    def cut(k):
        return pl.ds(pl.multiple_of(k * PIECE, PIECE), PIECE)

    def gate_copy(k):
        slot = lax.rem(k, DEPTH)
        return pltpu.make_async_copy(gate_ref.at[0, cut(k), :], gate.at[slot], sem_g.at[slot])

    def up_copy(k):
        slot = lax.rem(k, DEPTH)
        return pltpu.make_async_copy(up_ref.at[0, cut(k), :], up.at[slot], sem_u.at[slot])

    down_copy = pltpu.make_async_copy(down_ref.at[0], down, sem_d.at[0])
    loads = [
        pltpu.make_async_copy(in_ref.at[peers], msgs.at[side, peers], sem_m.at[side, i])
        for side, in_ref in enumerate((own_ref,))
        for i, peers in enumerate(CUTS)
    ]
    for load in loads:
        load.start()
    for k in range(DEPTH - 1):
        gate_copy(k).start()
        up_copy(k).start()
    core = core_ref[0]
    lane = iota((PAIRS, 128), 1)
    for side in range(2):
        flat = flats.at[side]
        for i, peers in enumerate(CUTS):
            if side == 0:
                loads[i].wait()
            arrived = other_ref[peers] if side else msgs[side, peers]
            flat.reshape(PAIRS, PITCH, 128)[peers, :MSG, :] = arrived.astype(F32)
        coef = flat[pl.ds(COEF_AT, PAIRS, stride=PITCH), :]
        for s in range(SLOTS):
            mine = jnp.where(lane // 2 == 2 * s + core, coef, 0.0)
            at = ROWS * side + PAIRS * s
            w_ref[at : at + PAIRS, :] = jnp.broadcast_to(jnp.sum(mine, axis=1, keepdims=True), (PAIRS, 128))
        lay_out(flat, rows.at[ROWS * side : ROWS * (side + 1)], 0, WIDE)
    acc[...] = jnp.zeros(acc.shape, F32)

    def piece(k, carry):
        slot = lax.rem(k, DEPTH)
        gate_copy(k).wait()
        up_copy(k).wait()

        @pl.when(k + DEPTH - 1 < PIECES)
        def _():
            gate_copy(k + DEPTH - 1).start()
            up_copy(k + DEPTH - 1).start()

        @pl.when(k + DEPTH - 1 == PIECES)
        def _():
            down_copy.start()

        part = rows[:, cut(k)]
        acc[:, :hidden] += jnp.dot(part, gate[slot], preferred_element_type=F32)
        acc[:, hidden:] += jnp.dot(part, up[slot], preferred_element_type=F32)
        return carry

    lax.fori_loop(0, PIECES, piece, 0)
    g, u = acc[:, :hidden], acc[:, hidden:]
    hid[...] = (g / (1.0 + jnp.exp(-g)) * u).astype(BF16)
    down_copy.wait()

    def columns(n, carry):
        value = jnp.dot(hid[...], down[:, cut(n)], preferred_element_type=F32)
        for m in range(PIECE // 128):
            part = value[:, lane_tile(m)] * w_ref[...]
            for s in range(2 * SLOTS):
                at = pl.ds(s % SLOTS * WIDE + PIECE // 128 * n + m, PAIRS, stride=PITCH)
                flats[s // SLOTS, at, :] = part[PAIRS * s : PAIRS * (s + 1)]
        return carry

    lax.fori_loop(0, PIECES, columns, 0)
    saves = []
    for side, out_ref in ((1, theirs_ref), (0, mine_ref)):
        for i, peers in enumerate(CUTS):
            msgs[side, peers] = flats.at[side].reshape(PAIRS, PITCH, 128)[peers, :MSG, :].astype(BF16)
            saves.append(pltpu.make_async_copy(msgs.at[side, peers], out_ref.at[peers], sem_m.at[side, i]))
            saves[-1].start()
    for save in saves:
        save.wait()


def fold_kernel(place_ref, *refs):
    parts, (total_ref, outs) = refs[:-5], (refs[-1], refs[-5:-1])
    total = parts[0][...].astype(F32)
    for part in parts[1:]:
        total = total + part[...].astype(F32)
    total_ref[...] = total
    size = total_ref.shape[0] // 4
    for flip, out_ref in enumerate(outs):
        at = jnp.bitwise_xor(place_ref[0], flip) * size
        out_ref[...] = total_ref[pl.ds(at, size)].astype(out_ref.dtype)


def mix_kernel(start, node_in, local_in, msg_in, *refs):
    before, (out_ref, flat_ref, rows_ref, node_ref, local_ref, msg_ref, sum_ref, sem) = refs[:-8], refs[-8:]
    loads = [(node_in, node_ref), (local_in, local_ref)]
    if before:
        loads += [(msg_in.at[cut], msg_ref.at[cut]) for cut in CUTS] + [(before[0], sum_ref)]
    copies = load_all(loads, sem)
    copies[0].wait()
    copies[1].wait()
    pick = jnp.concatenate(picks(node_ref, local_ref, start), axis=0).astype(BF16)
    for i, cut in enumerate(CUTS):
        if before:
            copies[2 + i].wait()
        arrived = msg_ref[cut] if before else msg_in[cut]
        flat_ref.reshape(PAIRS, PITCH, 128)[cut, :MSG, :] = arrived.astype(F32)
    lay_out(flat_ref, rows_ref, 0, WIDE)
    if before:
        copies[-1].wait()
    for k in range(7):
        at = slice(512 * k, 512 * (k + 1))
        value = lax.dot_general(pick, rows_ref[:, at], (((0,), (0,)), ((), ())), preferred_element_type=F32)
        if before:
            value = value + sum_ref[:, at]
        out_ref[:, at] = value.astype(out_ref.dtype)


def in_hbm(array):
    return pltpu.with_memory_space_constraint(array, pltpu.HBM)


def place(axes):
    return lax.axis_index(axes).astype(I32).reshape(1)


def vmem(mib):
    return pltpu.CompilerParams(vmem_limit_bytes=mib << 20)


def step(tokens, node_ids, local_ids, affinity, w_gate, w_up, w_down, grad_parts):
    tok, width = tokens.shape
    hidden = w_gate.shape[2]
    routes = node_ids.T, local_ids.T
    chips, swap = ("edp", "zh", "x", "y"), [(0, 1), (1, 0)]
    core = place("core")
    flat = pltpu.VMEM((PAIRS * PITCH, 128), F32)
    rows = pltpu.VMEM((ROWS, width), BF16)
    far, scalar = pl.BlockSpec(memory_space=pltpu.HBM), pl.BlockSpec(memory_space=pltpu.SMEM)
    local = pl.BlockSpec(memory_space=pltpu.VMEM)
    dma = pltpu.SemaphoreType.DMA
    small = [pltpu.VMEM((4, tok), I32), pltpu.VMEM((8, tok), I32)]

    def exchange(message):
        return lax.all_to_all(message, chips, split_axis=0, concat_axis=0, tiled=True)

    def send(start):
        shape = (PAIRS, MSG, 128)
        return pl.pallas_call(
            functools.partial(send_kernel, start),
            in_specs=[far] * 4,
            out_specs=far,
            out_shape=pltpu.HBM(shape, BF16),
            scratch_shapes=[flat, pltpu.VMEM(shape, BF16)]
            + small
            + [pltpu.VMEM((8, tok), F32), pltpu.VMEM((tok, width), BF16), dma((8,))],
            compiler_params=vmem(32),
            name="send",
        )(*map(in_hbm, (*routes, affinity.T, tokens)))

    def experts(own, other):
        shape = pltpu.HBM((PAIRS, MSG, 128), BF16)
        return pl.pallas_call(
            expert_kernel,
            in_specs=[scalar, far, local] + [far] * 3,
            out_specs=(far, far),
            out_shape=(shape, shape),
            scratch_shapes=[
                pltpu.VMEM((2, PAIRS, MSG, 128), BF16),
                dma((2, len(CUTS))),
                pltpu.VMEM((2, PAIRS * PITCH, 128), F32),
                pltpu.VMEM((2 * ROWS, width), BF16),
                pltpu.VMEM((DEPTH, PIECE, hidden), BF16),
                pltpu.VMEM((DEPTH, PIECE, hidden), BF16),
                pltpu.VMEM((hidden, width), BF16),
                pltpu.VMEM((2 * ROWS, 2 * hidden), F32),
                pltpu.VMEM((2 * ROWS, hidden), BF16),
                pltpu.VMEM((2 * ROWS, 128), F32),
                dma((DEPTH,)),
                dma((DEPTH,)),
                dma((1,)),
            ],
            compiler_params=vmem(50),
            cost_estimate=pl.CostEstimate(
                flops=12 * ROWS * width * hidden, bytes_accessed=6 * width * hidden + 16 * ROWS * width, transcendentals=0
            ),
            name="experts",
        )(core, in_hbm(own), other, *map(in_hbm, (w_gate, w_up, w_down)))

    def pair_result(message):
        other = lax.ppermute(message, "core", swap)
        mine, theirs = experts(message, other)
        back = lax.ppermute(theirs, "core", swap)
        return (mine.astype(F32) + back.astype(F32)).astype(BF16)

    def fold(axes, dtype, *parts):
        size = parts[0].shape[0] // 4
        shapes = [jax.ShapeDtypeStruct((size, GRAD, 128), F32)] + [jax.ShapeDtypeStruct((size, GRAD, 128), dtype)] * 3
        kept, *given = pl.pallas_call(
            fold_kernel,
            in_specs=[scalar] + [local] * len(parts),
            out_specs=[local] * 4,
            out_shape=shapes,
            scratch_shapes=[pltpu.VMEM(parts[0].shape, F32)],
            compiler_params=vmem(16),
            name="fold",
        )(place(axes), *parts)
        return [kept] + [
            lax.ppermute(part, axes, [(i, i ^ flip) for i in range(4)]) for flip, part in enumerate(given, 1)
        ]

    def mix(start, message, *before):
        return pl.pallas_call(
            functools.partial(mix_kernel, start),
            in_specs=[far, far] + ([far, far] if before else [local]),
            out_shape=jax.ShapeDtypeStruct((tok, width), BF16) if before else pltpu.HBM((tok, width), F32),
            scratch_shapes=[flat, rows]
            + small
            + [pltpu.VMEM((PAIRS, MSG, 128), BF16), pltpu.VMEM((tok, width), F32), dma((7,))],
            compiler_params=vmem(32),
            name="mix",
        )(*map(in_hbm, routes), in_hbm(message) if before else message, *map(in_hbm, before))

    halves = pl.pallas_call(
        halves_kernel,
        in_specs=[scalar, local],
        out_shape=(
            jax.ShapeDtypeStruct((PAIRS, GRAD, 128), F32),
            jax.ShapeDtypeStruct((PAIRS, GRAD, 128), BF16),
        ),
        compiler_params=vmem(32),
        name="halves",
    )
    keep, give = halves(core, grad_parts[0])
    got = lax.ppermute(give, "core", swap)
    parts = fold(("edp", "zh"), BF16, keep, got)
    parts = fold("x", F32, *parts)
    parts = fold("y", F32, *parts)
    total = (parts[0] + parts[1] + parts[2] + parts[3])[0]
    low = total[:WIDE]
    high = jnp.concatenate([total[WIDE:], total[:24]], axis=0)
    router_grad = jnp.where(core[0] == 0, low, high)
    message = send(0)
    arrived = exchange(message)
    message_2 = send(SLOTS)
    arrived_2 = exchange(message_2)
    result = pair_result(arrived)
    returned = exchange(result)
    result_2 = pair_result(arrived_2)
    returned_2 = exchange(result_2)
    partial = mix(0, returned)
    return mix(SLOTS, returned_2, partial), router_grad


def solution(mesh):
    axes = ("edp", "zh", "x", "y", "core")
    split = Mesh(mesh.devices.reshape(2, 2, 4, 4, 2), axes)
    flat, deep = P(axes, None), P(axes, None, None)
    return jax.shard_map(
        step,
        mesh=split,
        in_specs=(flat, flat, flat, flat, deep, deep, deep, deep),
        out_specs=(flat, flat),
        check_vma=False,
    )
```

```python
import functools

import jax
import jax.numpy as jnp
from jax import lax
from jax.experimental import pallas as pl
from jax.experimental.pallas import tpu as pltpu
from jax.sharding import Mesh, PartitionSpec as P


PAIRS, SLOTS, WIDE = 64, 5, 28
COEF_AT = SLOTS * WIDE
MSG = COEF_AT + 4
GRAD = 32
PITCH = MSG + 8
ROWS = PAIRS * SLOTS
CUTS = tuple(slice(16 * i, 16 * (i + 1)) for i in range(PAIRS // 16))
F32, BF16, I32 = jnp.float32, jnp.bfloat16, jnp.int32


def iota(shape, dim):
    return lax.broadcasted_iota(I32, shape, dim)


def pair_of(node_ref, local_ref, column):
    return node_ref[column : column + 1, :] * 8 + local_ref[2 * column : 2 * column + 1, :] // 2


def picks(node_ref, local_ref, start):
    tok = node_ref.shape[1]
    pair = iota((PAIRS, tok), 0)
    hit = jnp.zeros((PAIRS, tok), jnp.bool_)
    for column in range(4):
        hit = hit | (pair == pair_of(node_ref, local_ref, column))
    earlier = (iota((tok, tok), 0) < iota((tok, tok), 1)).astype(BF16)
    rank = jnp.dot(hit.astype(F32).astype(BF16), earlier, preferred_element_type=F32)
    return [jnp.where(hit & (rank == float(start + slot)), 1.0, 0.0) for slot in range(SLOTS)]


def lane_tile(j):
    return slice(128 * j, 128 * (j + 1))


def load_all(pairs, sem):
    copies = [pltpu.make_async_copy(src, dst, sem.at[i]) for i, (src, dst) in enumerate(pairs)]
    for copy in copies:
        copy.start()
    return copies


def send_kernel(start, node_in, local_in, aff_in, tok_in, *refs):
    grad_refs, (out_ref, flat_ref, stage_ref, node_ref, local_ref, aff_ref, tok_ref, sem) = refs[:-8], refs[-8:]
    here = ((node_in, node_ref), (local_in, local_ref), (aff_in, aff_ref), (tok_in, tok_ref))
    copies = load_all(here, sem)
    for copy in copies[:3]:
        copy.wait()
    each = picks(node_ref, local_ref, start)
    pick = jnp.concatenate(each, axis=0).astype(BF16)
    copies[3].wait()
    for k in range(7):
        rows = jnp.dot(pick, tok_ref[:, 512 * k : 512 * (k + 1)], preferred_element_type=F32)
        for m in range(4):
            for s in range(SLOTS):
                at = pl.ds(s * WIDE + 4 * k + m, PAIRS, stride=PITCH)
                flat_ref[at, :] = rows[PAIRS * s : PAIRS * (s + 1), lane_tile(m)]
    aff = aff_ref[...]
    weight = 2.5 * aff / jnp.sum(aff, axis=0, keepdims=True)
    tok = node_ref.shape[1]
    pair = iota((PAIRS, tok), 0)
    even = jnp.zeros((PAIRS, tok), F32)
    odd = jnp.zeros((PAIRS, tok), F32)
    for column in range(4):
        first, second = weight[2 * column : 2 * column + 1, :], weight[2 * column + 1 : 2 * column + 2, :]
        flip = local_ref[2 * column : 2 * column + 1, :] % 2 == 1
        here = pair == pair_of(node_ref, local_ref, column)
        even = jnp.where(here, jnp.where(flip, second, first), even)
        odd = jnp.where(here, jnp.where(flip, first, second), odd)
    lane = iota((PAIRS, 128), 1)
    coef = jnp.zeros((PAIRS, 128), F32)
    for slot in range(SLOTS):
        even_w = jnp.sum(each[slot] * even, axis=1, keepdims=True)
        odd_w = jnp.sum(each[slot] * odd, axis=1, keepdims=True)
        coef = jnp.where(lane // 2 == 2 * slot, even_w, coef)
        coef = jnp.where(lane // 2 == 2 * slot + 1, odd_w, coef)
    high = coef.astype(BF16).astype(F32)
    coef = jnp.where(lane % 2 == 0, high, coef - high)
    for row in range(COEF_AT, MSG):
        flat_ref[pl.ds(row, PAIRS, stride=PITCH), :] = coef
    saves = []
    for i, cut in enumerate(CUTS):
        stage_ref[cut, :MSG, :] = flat_ref.reshape(PAIRS, PITCH, 128)[cut, :MSG, :].astype(BF16)
        if grad_refs:
            keep_ref, got_ref = grad_refs
            stage_ref[cut, MSG:, :] = (keep_ref[cut] + got_ref[cut].astype(F32)).astype(BF16)
        saves.append(pltpu.make_async_copy(stage_ref.at[cut], out_ref.at[cut], sem.at[4 + i]))
        saves[-1].start()
    for save in saves:
        save.wait()


def halves_kernel(core_ref, in_ref, keep_ref, give_ref):
    blocks = in_ref.reshape(PAIRS, 2 * WIDE, 128)
    first = core_ref[0] == 0
    low, high = blocks[:, :24, :], blocks[:, 32:, :]
    shared = blocks[:, 24:32, :]
    keep_ref[:, :24, :] = jnp.where(first, low, high)
    keep_ref[:, 24:, :] = shared
    give_ref[:, :24, :] = jnp.where(first, high, low).astype(BF16)
    give_ref[:, 24:, :] = shared.astype(BF16)


def spread(src_ref, flat_ref):
    flat_ref.reshape(PAIRS, PITCH, 128)[:, :MSG, :] = src_ref[:, :MSG, :].astype(F32)


def lay_out(flat_ref, rows_ref, first, last):
    for s in range(SLOTS):
        for j in range(first, last):
            tile = flat_ref[pl.ds(s * WIDE + j, PAIRS, stride=PITCH), :]
            rows_ref[PAIRS * s : PAIRS * (s + 1), lane_tile(j)] = tile.astype(BF16)


PIECE, PIECES, DEPTH = 512, 7, 4


def expert_kernel(
    core_ref, own_ref, other_ref, gate_ref, up_ref, down_ref, mine_ref, theirs_ref,
    flats, rows, gate, up, down, acc, hid, w_ref, sem_g, sem_u, sem_d,
):
    hidden = gate.shape[2]

    def cut(k):
        return pl.ds(pl.multiple_of(k * PIECE, PIECE), PIECE)

    def gate_copy(k):
        slot = lax.rem(k, DEPTH)
        return pltpu.make_async_copy(gate_ref.at[0, cut(k), :], gate.at[slot], sem_g.at[slot])

    def up_copy(k):
        slot = lax.rem(k, DEPTH)
        return pltpu.make_async_copy(up_ref.at[0, cut(k), :], up.at[slot], sem_u.at[slot])

    down_copy = pltpu.make_async_copy(down_ref.at[0], down, sem_d.at[0])
    for k in range(DEPTH - 1):
        gate_copy(k).start()
        up_copy(k).start()
    core = core_ref[0]
    lane = iota((PAIRS, 128), 1)
    for side, in_ref in enumerate((own_ref, other_ref)):
        flat = flats.at[side]
        spread(in_ref, flat)
        coef = flat[pl.ds(COEF_AT, PAIRS, stride=PITCH), :]
        for s in range(SLOTS):
            mine = jnp.where(lane // 2 == 2 * s + core, coef, 0.0)
            at = ROWS * side + PAIRS * s
            w_ref[at : at + PAIRS, :] = jnp.broadcast_to(jnp.sum(mine, axis=1, keepdims=True), (PAIRS, 128))
        lay_out(flat, rows.at[ROWS * side : ROWS * (side + 1)], 0, WIDE)
    acc[...] = jnp.zeros(acc.shape, F32)

    def piece(k, carry):
        slot = lax.rem(k, DEPTH)
        gate_copy(k).wait()
        up_copy(k).wait()

        @pl.when(k + DEPTH - 1 < PIECES)
        def _():
            gate_copy(k + DEPTH - 1).start()
            up_copy(k + DEPTH - 1).start()

        @pl.when(k + DEPTH - 1 == PIECES)
        def _():
            down_copy.start()

        part = rows[:, cut(k)]
        acc[:, :hidden] += jnp.dot(part, gate[slot], preferred_element_type=F32)
        acc[:, hidden:] += jnp.dot(part, up[slot], preferred_element_type=F32)
        return carry

    lax.fori_loop(0, PIECES, piece, 0)
    g, u = acc[:, :hidden], acc[:, hidden:]
    hid[...] = (g / (1.0 + jnp.exp(-g)) * u).astype(BF16)
    down_copy.wait()

    def columns(n, carry):
        value = jnp.dot(hid[...], down[:, cut(n)], preferred_element_type=F32)
        for m in range(PIECE // 128):
            part = value[:, lane_tile(m)] * w_ref[...]
            for s in range(2 * SLOTS):
                at = pl.ds(s % SLOTS * WIDE + PIECE // 128 * n + m, PAIRS, stride=PITCH)
                flats[s // SLOTS, at, :] = part[PAIRS * s : PAIRS * (s + 1)]
        return carry

    lax.fori_loop(0, PIECES, columns, 0)
    for side, out_ref in enumerate((mine_ref, theirs_ref)):
        out_ref[...] = flats.at[side].reshape(PAIRS, PITCH, 128)[:, :MSG, :].astype(BF16)


def mix_kernel(start, node_in, local_in, msg_in, *refs):
    before, (out_ref, flat_ref, rows_ref, node_ref, local_ref, msg_ref, sum_ref, sem) = refs[:-8], refs[-8:]
    loads = [(node_in, node_ref), (local_in, local_ref)]
    if before:
        loads += [(msg_in.at[cut], msg_ref.at[cut]) for cut in CUTS] + [(before[0], sum_ref)]
    copies = load_all(loads, sem)
    copies[0].wait()
    copies[1].wait()
    pick = jnp.concatenate(picks(node_ref, local_ref, start), axis=0).astype(BF16)
    for i, cut in enumerate(CUTS):
        if before:
            copies[2 + i].wait()
        arrived = msg_ref[cut] if before else msg_in[cut]
        flat_ref.reshape(PAIRS, PITCH, 128)[cut, :MSG, :] = arrived.astype(F32)
    lay_out(flat_ref, rows_ref, 0, WIDE)
    if before:
        copies[-1].wait()
    for k in range(7):
        at = slice(512 * k, 512 * (k + 1))
        value = lax.dot_general(pick, rows_ref[:, at], (((0,), (0,)), ((), ())), preferred_element_type=F32)
        if before:
            value = value + sum_ref[:, at]
        out_ref[:, at] = value.astype(out_ref.dtype)


def in_hbm(array):
    return pltpu.with_memory_space_constraint(array, pltpu.HBM)


def place(axes):
    return lax.axis_index(axes).astype(I32).reshape(1)


def vmem(mib):
    return pltpu.CompilerParams(vmem_limit_bytes=mib << 20)


def step(tokens, node_ids, local_ids, affinity, w_gate, w_up, w_down, grad_parts):
    tok, width = tokens.shape
    hidden = w_gate.shape[2]
    routes = node_ids.T, local_ids.T
    chips, swap = ("edp", "zh", "x", "y"), [(0, 1), (1, 0)]
    core = place("core")
    flat = pltpu.VMEM((PAIRS * PITCH, 128), F32)
    rows = pltpu.VMEM((ROWS, width), BF16)
    far, scalar = pl.BlockSpec(memory_space=pltpu.HBM), pl.BlockSpec(memory_space=pltpu.SMEM)
    local = pl.BlockSpec(memory_space=pltpu.VMEM)
    dma = pltpu.SemaphoreType.DMA
    small = [pltpu.VMEM((4, tok), I32), pltpu.VMEM((8, tok), I32)]

    def exchange(message):
        return lax.all_to_all(message, chips, split_axis=0, concat_axis=0, tiled=True)

    def send(start, *grads):
        shape = (PAIRS, MSG + (GRAD if grads else 0), 128)
        return pl.pallas_call(
            functools.partial(send_kernel, start),
            in_specs=[far] * 4 + [local] * len(grads),
            out_specs=far,
            out_shape=pltpu.HBM(shape, BF16),
            scratch_shapes=[flat, pltpu.VMEM(shape, BF16)]
            + small
            + [pltpu.VMEM((8, tok), F32), pltpu.VMEM((tok, width), BF16), dma((8,))],
            compiler_params=vmem(32),
            name="send",
        )(*map(in_hbm, (*routes, affinity.T, tokens)), *grads)

    def experts(own, other):
        shape = jax.ShapeDtypeStruct((PAIRS, MSG, 128), BF16)
        return pl.pallas_call(
            expert_kernel,
            in_specs=[scalar, local, local] + [far] * 3,
            out_specs=(local, local),
            out_shape=(shape, shape),
            scratch_shapes=[
                pltpu.VMEM((2, PAIRS * PITCH, 128), F32),
                pltpu.VMEM((2 * ROWS, width), BF16),
                pltpu.VMEM((DEPTH, PIECE, hidden), BF16),
                pltpu.VMEM((DEPTH, PIECE, hidden), BF16),
                pltpu.VMEM((hidden, width), BF16),
                pltpu.VMEM((2 * ROWS, 2 * hidden), F32),
                pltpu.VMEM((2 * ROWS, hidden), BF16),
                pltpu.VMEM((2 * ROWS, 128), F32),
                dma((DEPTH,)),
                dma((DEPTH,)),
                dma((1,)),
            ],
            compiler_params=vmem(46),
            cost_estimate=pl.CostEstimate(
                flops=12 * ROWS * width * hidden, bytes_accessed=6 * width * hidden + 16 * ROWS * width, transcendentals=0
            ),
            name="experts",
        )(core, own, other, *map(in_hbm, (w_gate, w_up, w_down)))

    def pair_result(message):
        other = lax.ppermute(message, "core", swap)
        mine, theirs = experts(message, other)
        back = lax.ppermute(theirs, "core", swap)
        return (mine.astype(F32) + back.astype(F32)).astype(BF16)

    def mix(start, message, *before):
        return pl.pallas_call(
            functools.partial(mix_kernel, start),
            in_specs=[far, far] + ([far, far] if before else [local]),
            out_shape=jax.ShapeDtypeStruct((tok, width), BF16) if before else pltpu.HBM((tok, width), F32),
            scratch_shapes=[flat, rows]
            + small
            + [pltpu.VMEM((PAIRS, MSG, 128), BF16), pltpu.VMEM((tok, width), F32), dma((7,))],
            compiler_params=vmem(32),
            name="mix",
        )(*map(in_hbm, routes), in_hbm(message) if before else message, *map(in_hbm, before))

    halves = pl.pallas_call(
        halves_kernel,
        in_specs=[scalar, local],
        out_shape=(
            jax.ShapeDtypeStruct((PAIRS, GRAD, 128), F32),
            jax.ShapeDtypeStruct((PAIRS, GRAD, 128), BF16),
        ),
        compiler_params=vmem(32),
        name="halves",
    )
    keep, give = halves(core, grad_parts[0])
    got = lax.ppermute(give, "core", swap)
    message = send(0)
    arrived = exchange(message)
    message_2 = send(SLOTS, keep, got)
    arrived_2 = exchange(message_2)
    result = pair_result(arrived)
    returned = exchange(result)
    result_2 = pair_result(arrived_2)
    returned_2 = exchange(result_2)
    partial = mix(0, returned)
    mixed = mix(SLOTS, returned_2, partial)
    total = jnp.sum(arrived_2[:, MSG:, :].astype(F32), axis=0)
    high = jnp.concatenate([total[WIDE:], total[:24]], axis=0)
    return mixed, jnp.where(core[0] == 0, total[:WIDE], high)


def solution(mesh):
    axes = ("edp", "zh", "x", "y", "core")
    split = Mesh(mesh.devices.reshape(2, 2, 4, 4, 2), axes)
    flat, deep = P(axes, None), P(axes, None, None)
    return jax.shard_map(
        step,
        mesh=split,
        in_specs=(flat, flat, flat, flat, deep, deep, deep, deep),
        out_specs=(flat, flat),
        check_vma=False,
    )
```

```python
import functools

import jax
import jax.numpy as jnp
from jax import lax
from jax.experimental import pallas as pl
from jax.experimental.pallas import tpu as pltpu
from jax.sharding import Mesh, PartitionSpec as P


PAIRS, SLOTS, WIDE = 64, 5, 28
COEF_AT = SLOTS * WIDE
MSG = COEF_AT + 4
GRAD = 32
PITCH = MSG + 8
ROWS = PAIRS * SLOTS
CUTS = tuple(slice(16 * i, 16 * (i + 1)) for i in range(PAIRS // 16))
F32, BF16, I32 = jnp.float32, jnp.bfloat16, jnp.int32


def iota(shape, dim):
    return lax.broadcasted_iota(I32, shape, dim)


def pair_of(node_ref, local_ref, column):
    return node_ref[column : column + 1, :] * 8 + local_ref[2 * column : 2 * column + 1, :] // 2


def picks(node_ref, local_ref, start):
    tok = node_ref.shape[1]
    pair = iota((PAIRS, tok), 0)
    hit = jnp.zeros((PAIRS, tok), jnp.bool_)
    for column in range(4):
        hit = hit | (pair == pair_of(node_ref, local_ref, column))
    earlier = (iota((tok, tok), 0) < iota((tok, tok), 1)).astype(BF16)
    rank = jnp.dot(hit.astype(F32).astype(BF16), earlier, preferred_element_type=F32)
    return [jnp.where(hit & (rank == float(start + slot)), 1.0, 0.0) for slot in range(SLOTS)]


def lane_tile(j):
    return slice(128 * j, 128 * (j + 1))


def load_all(pairs, sem):
    copies = [pltpu.make_async_copy(src, dst, sem.at[i]) for i, (src, dst) in enumerate(pairs)]
    for copy in copies:
        copy.start()
    return copies


def send_kernel(
    start, node_in, local_in, aff_in, tok_in, out_ref, flat_ref, stage_ref, node_ref, local_ref, aff_ref, tok_ref, sem
):
    here = ((node_in, node_ref), (local_in, local_ref), (aff_in, aff_ref), (tok_in, tok_ref))
    copies = load_all(here, sem)
    for copy in copies[:3]:
        copy.wait()
    each = picks(node_ref, local_ref, start)
    pick = jnp.concatenate(each, axis=0).astype(BF16)
    copies[3].wait()
    for k in range(7):
        rows = jnp.dot(pick, tok_ref[:, 512 * k : 512 * (k + 1)], preferred_element_type=F32)
        for m in range(4):
            for s in range(SLOTS):
                at = pl.ds(s * WIDE + 4 * k + m, PAIRS, stride=PITCH)
                flat_ref[at, :] = rows[PAIRS * s : PAIRS * (s + 1), lane_tile(m)]
    aff = aff_ref[...]
    weight = 2.5 * aff / jnp.sum(aff, axis=0, keepdims=True)
    tok = node_ref.shape[1]
    pair = iota((PAIRS, tok), 0)
    even = jnp.zeros((PAIRS, tok), F32)
    odd = jnp.zeros((PAIRS, tok), F32)
    for column in range(4):
        first, second = weight[2 * column : 2 * column + 1, :], weight[2 * column + 1 : 2 * column + 2, :]
        flip = local_ref[2 * column : 2 * column + 1, :] % 2 == 1
        here = pair == pair_of(node_ref, local_ref, column)
        even = jnp.where(here, jnp.where(flip, second, first), even)
        odd = jnp.where(here, jnp.where(flip, first, second), odd)
    lane = iota((PAIRS, 128), 1)
    coef = jnp.zeros((PAIRS, 128), F32)
    for slot in range(SLOTS):
        even_w = jnp.sum(each[slot] * even, axis=1, keepdims=True)
        odd_w = jnp.sum(each[slot] * odd, axis=1, keepdims=True)
        coef = jnp.where(lane // 2 == 2 * slot, even_w, coef)
        coef = jnp.where(lane // 2 == 2 * slot + 1, odd_w, coef)
    high = coef.astype(BF16).astype(F32)
    coef = jnp.where(lane % 2 == 0, high, coef - high)
    for row in range(COEF_AT, MSG):
        flat_ref[pl.ds(row, PAIRS, stride=PITCH), :] = coef
    saves = []
    for i, cut in enumerate(CUTS):
        stage_ref[cut] = flat_ref.reshape(PAIRS, PITCH, 128)[cut, :MSG, :].astype(BF16)
        saves.append(pltpu.make_async_copy(stage_ref.at[cut], out_ref.at[cut], sem.at[4 + i]))
        saves[-1].start()
    for save in saves:
        save.wait()


def halves_kernel(core_ref, in_ref, keep_ref, give_ref):
    blocks = in_ref.reshape(PAIRS, 2 * WIDE, 128)
    first = core_ref[0] == 0
    low, high = blocks[:, :24, :], blocks[:, 32:, :]
    shared = blocks[:, 24:32, :]
    keep_ref[:, :24, :] = jnp.where(first, low, high)
    keep_ref[:, 24:, :] = shared
    give_ref[:, :24, :] = jnp.where(first, high, low).astype(BF16)
    give_ref[:, 24:, :] = shared.astype(BF16)


def spread(src_ref, flat_ref):
    flat_ref.reshape(PAIRS, PITCH, 128)[:, :MSG, :] = src_ref[:, :MSG, :].astype(F32)


def lay_out(flat_ref, rows_ref, first, last):
    for s in range(SLOTS):
        for j in range(first, last):
            tile = flat_ref[pl.ds(s * WIDE + j, PAIRS, stride=PITCH), :]
            rows_ref[PAIRS * s : PAIRS * (s + 1), lane_tile(j)] = tile.astype(BF16)


PIECE, PIECES, DEPTH = 512, 7, 4


def expert_kernel(
    core_ref, own_ref, other_ref, gate_ref, up_ref, down_ref, mine_ref, theirs_ref,
    flats, rows, gate, up, down, acc, hid, w_ref, sem_g, sem_u, sem_d,
):
    hidden = gate.shape[2]

    def cut(k):
        return pl.ds(pl.multiple_of(k * PIECE, PIECE), PIECE)

    def gate_copy(k):
        slot = lax.rem(k, DEPTH)
        return pltpu.make_async_copy(gate_ref.at[0, cut(k), :], gate.at[slot], sem_g.at[slot])

    def up_copy(k):
        slot = lax.rem(k, DEPTH)
        return pltpu.make_async_copy(up_ref.at[0, cut(k), :], up.at[slot], sem_u.at[slot])

    down_copy = pltpu.make_async_copy(down_ref.at[0], down, sem_d.at[0])
    for k in range(DEPTH - 1):
        gate_copy(k).start()
        up_copy(k).start()
    core = core_ref[0]
    lane = iota((PAIRS, 128), 1)
    for side, in_ref in enumerate((own_ref, other_ref)):
        flat = flats.at[side]
        spread(in_ref, flat)
        coef = flat[pl.ds(COEF_AT, PAIRS, stride=PITCH), :]
        for s in range(SLOTS):
            mine = jnp.where(lane // 2 == 2 * s + core, coef, 0.0)
            at = ROWS * side + PAIRS * s
            w_ref[at : at + PAIRS, :] = jnp.broadcast_to(jnp.sum(mine, axis=1, keepdims=True), (PAIRS, 128))
        lay_out(flat, rows.at[ROWS * side : ROWS * (side + 1)], 0, WIDE)
    acc[...] = jnp.zeros(acc.shape, F32)

    def piece(k, carry):
        slot = lax.rem(k, DEPTH)
        gate_copy(k).wait()
        up_copy(k).wait()

        @pl.when(k + DEPTH - 1 < PIECES)
        def _():
            gate_copy(k + DEPTH - 1).start()
            up_copy(k + DEPTH - 1).start()

        @pl.when(k + DEPTH - 1 == PIECES)
        def _():
            down_copy.start()

        part = rows[:, cut(k)]
        acc[:, :hidden] += jnp.dot(part, gate[slot], preferred_element_type=F32)
        acc[:, hidden:] += jnp.dot(part, up[slot], preferred_element_type=F32)
        return carry

    lax.fori_loop(0, PIECES, piece, 0)
    g, u = acc[:, :hidden], acc[:, hidden:]
    hid[...] = (g / (1.0 + jnp.exp(-g)) * u).astype(BF16)
    down_copy.wait()

    def columns(n, carry):
        value = jnp.dot(hid[...], down[:, cut(n)], preferred_element_type=F32)
        for m in range(PIECE // 128):
            part = value[:, lane_tile(m)] * w_ref[...]
            for s in range(2 * SLOTS):
                at = pl.ds(s % SLOTS * WIDE + PIECE // 128 * n + m, PAIRS, stride=PITCH)
                flats[s // SLOTS, at, :] = part[PAIRS * s : PAIRS * (s + 1)]
        return carry

    lax.fori_loop(0, PIECES, columns, 0)
    for side, out_ref in enumerate((mine_ref, theirs_ref)):
        out_ref[...] = flats.at[side].reshape(PAIRS, PITCH, 128)[:, :MSG, :].astype(BF16)


def fold_kernel(place_ref, *refs):
    parts, (outs, stages, sem) = refs[:-9], (refs[-9:-5], refs[-5:-1], refs[-1])
    size = outs[0].shape[0]
    saves = []
    for flip in range(4):
        at = pl.ds(jnp.bitwise_xor(place_ref[0], flip) * size, size)
        total = parts[0][at].astype(F32)
        for part in parts[1:]:
            total = total + part[at].astype(F32)
        stages[flip][...] = total.astype(stages[flip].dtype)
        saves.append(pltpu.make_async_copy(stages[flip], outs[flip], sem.at[flip]))
        saves[-1].start()
    for save in saves:
        save.wait()


def mix_kernel(start, node_in, local_in, msg_in, *refs):
    before, (out_ref, flat_ref, rows_ref, node_ref, local_ref, msg_ref, sum_ref, sem) = refs[:-8], refs[-8:]
    loads = [(node_in, node_ref), (local_in, local_ref)]
    if before:
        loads += [(msg_in.at[cut], msg_ref.at[cut]) for cut in CUTS] + [(before[0], sum_ref)]
    copies = load_all(loads, sem)
    copies[0].wait()
    copies[1].wait()
    pick = jnp.concatenate(picks(node_ref, local_ref, start), axis=0).astype(BF16)
    for i, cut in enumerate(CUTS):
        if before:
            copies[2 + i].wait()
        arrived = msg_ref[cut] if before else msg_in[cut]
        flat_ref.reshape(PAIRS, PITCH, 128)[cut, :MSG, :] = arrived.astype(F32)
    lay_out(flat_ref, rows_ref, 0, WIDE)
    if before:
        copies[-1].wait()
    for k in range(7):
        at = slice(512 * k, 512 * (k + 1))
        value = lax.dot_general(pick, rows_ref[:, at], (((0,), (0,)), ((), ())), preferred_element_type=F32)
        if before:
            value = value + sum_ref[:, at]
        out_ref[:, at] = value.astype(out_ref.dtype)


def in_hbm(array):
    return pltpu.with_memory_space_constraint(array, pltpu.HBM)


def place(axes):
    return lax.axis_index(axes).astype(I32).reshape(1)


def vmem(mib):
    return pltpu.CompilerParams(vmem_limit_bytes=mib << 20)


def step(tokens, node_ids, local_ids, affinity, w_gate, w_up, w_down, grad_parts):
    tok, width = tokens.shape
    hidden = w_gate.shape[2]
    routes = node_ids.T, local_ids.T
    chips, swap = ("edp", "zh", "x", "y"), [(0, 1), (1, 0)]
    core = place("core")
    flat = pltpu.VMEM((PAIRS * PITCH, 128), F32)
    rows = pltpu.VMEM((ROWS, width), BF16)
    far, scalar = pl.BlockSpec(memory_space=pltpu.HBM), pl.BlockSpec(memory_space=pltpu.SMEM)
    local = pl.BlockSpec(memory_space=pltpu.VMEM)
    dma = pltpu.SemaphoreType.DMA
    small = [pltpu.VMEM((4, tok), I32), pltpu.VMEM((8, tok), I32)]

    def exchange(message):
        return lax.all_to_all(message, chips, split_axis=0, concat_axis=0, tiled=True)

    def send(start):
        shape = (PAIRS, MSG, 128)
        return pl.pallas_call(
            functools.partial(send_kernel, start),
            in_specs=[far] * 4,
            out_specs=far,
            out_shape=pltpu.HBM(shape, BF16),
            scratch_shapes=[flat, pltpu.VMEM(shape, BF16)]
            + small
            + [pltpu.VMEM((8, tok), F32), pltpu.VMEM((tok, width), BF16), dma((8,))],
            compiler_params=vmem(32),
            name="send",
        )(*map(in_hbm, (*routes, affinity.T, tokens)))

    def experts(own, other):
        shape = jax.ShapeDtypeStruct((PAIRS, MSG, 128), BF16)
        return pl.pallas_call(
            expert_kernel,
            in_specs=[scalar, local, local] + [far] * 3,
            out_specs=(local, local),
            out_shape=(shape, shape),
            scratch_shapes=[
                pltpu.VMEM((2, PAIRS * PITCH, 128), F32),
                pltpu.VMEM((2 * ROWS, width), BF16),
                pltpu.VMEM((DEPTH, PIECE, hidden), BF16),
                pltpu.VMEM((DEPTH, PIECE, hidden), BF16),
                pltpu.VMEM((hidden, width), BF16),
                pltpu.VMEM((2 * ROWS, 2 * hidden), F32),
                pltpu.VMEM((2 * ROWS, hidden), BF16),
                pltpu.VMEM((2 * ROWS, 128), F32),
                dma((DEPTH,)),
                dma((DEPTH,)),
                dma((1,)),
            ],
            compiler_params=vmem(46),
            cost_estimate=pl.CostEstimate(
                flops=12 * ROWS * width * hidden, bytes_accessed=6 * width * hidden + 16 * ROWS * width, transcendentals=0
            ),
            name="experts",
        )(core, own, other, *map(in_hbm, (w_gate, w_up, w_down)))

    def pair_result(message):
        other = lax.ppermute(message, "core", swap)
        mine, theirs = experts(message, other)
        back = lax.ppermute(theirs, "core", swap)
        return (mine.astype(F32) + back.astype(F32)).astype(BF16)

    def fold(axes, dtype, *parts):
        shape = (parts[0].shape[0] // 4, GRAD, 128)
        kinds = (F32, dtype, dtype, dtype)
        kept, *given = pl.pallas_call(
            fold_kernel,
            in_specs=[scalar] + [local] * len(parts),
            out_specs=[far] * 4,
            out_shape=[pltpu.HBM(shape, kind) for kind in kinds],
            scratch_shapes=[pltpu.VMEM(shape, kind) for kind in kinds] + [dma((4,))],
            compiler_params=vmem(16),
            name="fold",
        )(place(axes), *parts)
        return [kept] + [
            lax.ppermute(part, axes, [(i, i ^ flip) for i in range(4)]) for flip, part in enumerate(given, 1)
        ]

    def mix(start, message, *before):
        return pl.pallas_call(
            functools.partial(mix_kernel, start),
            in_specs=[far, far] + ([far, far] if before else [local]),
            out_shape=jax.ShapeDtypeStruct((tok, width), BF16) if before else pltpu.HBM((tok, width), F32),
            scratch_shapes=[flat, rows]
            + small
            + [pltpu.VMEM((PAIRS, MSG, 128), BF16), pltpu.VMEM((tok, width), F32), dma((7,))],
            compiler_params=vmem(32),
            name="mix",
        )(*map(in_hbm, routes), in_hbm(message) if before else message, *map(in_hbm, before))

    halves = pl.pallas_call(
        halves_kernel,
        in_specs=[scalar, local],
        out_shape=(
            jax.ShapeDtypeStruct((PAIRS, GRAD, 128), F32),
            jax.ShapeDtypeStruct((PAIRS, GRAD, 128), BF16),
        ),
        compiler_params=vmem(32),
        name="halves",
    )
    keep, give = halves(core, grad_parts[0])
    got = lax.ppermute(give, "core", swap)
    parts = fold(("edp", "zh"), BF16, keep, got)
    parts = fold("x", F32, *parts)
    parts = fold("y", F32, *parts)
    total = (parts[0] + parts[1] + parts[2] + parts[3])[0]
    low = total[:WIDE]
    high = jnp.concatenate([total[WIDE:], total[:24]], axis=0)
    router_grad = jnp.where(core[0] == 0, low, high)
    message = send(0)
    arrived = exchange(message)
    message_2 = send(SLOTS)
    arrived_2 = exchange(message_2)
    result = pair_result(arrived)
    returned = exchange(result)
    result_2 = pair_result(arrived_2)
    returned_2 = exchange(result_2)
    partial = mix(0, returned)
    return mix(SLOTS, returned_2, partial), router_grad


def solution(mesh):
    axes = ("edp", "zh", "x", "y", "core")
    split = Mesh(mesh.devices.reshape(2, 2, 4, 4, 2), axes)
    flat, deep = P(axes, None), P(axes, None, None)
    return jax.shard_map(
        step,
        mesh=split,
        in_specs=(flat, flat, flat, flat, deep, deep, deep, deep),
        out_specs=(flat, flat),
        check_vma=False,
    )
```
